32 devices in a mesh: dom: 8 (over y, x, core), sub: 4 (over z).
Axes of the slice: x: 2, y: 2, z: 4, core: 2. Of those that a mesh axis runs over, the one named last changes fastest.
Arguments:
- features: bfloat16 [32768, 602], P(('dom', 'sub')), may hold values from -6 to 6
- w_inner: bfloat16 [602, 256], replicated, may hold values from -0.25 to 0.25
- bias_inner: float32 [256], replicated, may hold values from -6 to 6
- w_outer: bfloat16 [256, 41], replicated, may hold values from -0.375 to 0.375
- bias_outer: float32 [41], replicated, may hold values from -6 to 6
- tiles: bfloat16 [256, 32, 128, 128], P(('dom', 'sub')), may hold values from -3 to 3
- tile_col: int32 [256, 32], P(('dom', 'sub')), may hold values from 0 to 39, as said below
- degrees: int32 [32768], P(('dom', 'sub')), may hold values from 1 to 32
- send_rows: int32 [32, 32, 128], P(('dom', 'sub')), may hold values from -1 to 1023, as said below
Outputs:
- logits: float32 [32768, 41], P(('dom', 'sub'))
The draws below stay inside these ranges and needn't reach their ends.
Inputs may be any that keep to these rules, and one draw needn't show every extreme that they name: send_rows[e, p, s] is the row, among device e's 1024 vertices, that fills slot s of e's list for device p, or -1 for an unused slot; live slots come first and every list has 1 to 128 live slots; every sender has a full list, and in every draw some device receives full lists from all senders. tile_col[d * 8 + r, t] is the column block, in device d's column space, of tile t of row block r; the 32 column blocks of a row block are distinct.
All inputs are finite; a program needn't handle non-finite values.
Results may differ from the reference program's by a relative error of at most 0.0042.
Values may be sent and summed in bfloat16 or wider, within the bound.
A program may use at most 128 MiB of HBM per device.

```python
import jax
import jax.numpy as jnp
from jax import lax

F_IN = 602
HID = 256
CLASSES = 41
BLK = 128
TILES = 32
V_DEV = 1024
PEERS = 32
ROW_BLOCKS = 8
COL_BLOCKS = 40
VERTS = 32768


def draw_send_rows(key, part):
    key_rows = jax.random.fold_in(key, 11)
    key_counts = jax.random.fold_in(key, 12)
    key_full = jax.random.fold_in(key, 13)
    key_target = jax.random.fold_in(key, 14)
    picked = jax.random.randint(key_rows, (PEERS, PEERS, BLK), 0, V_DEV)
    counts = jax.random.randint(key_counts, (PEERS, PEERS), 1, BLK + 1)
    full_peer = jax.random.randint(key_full, (PEERS,), 0, PEERS)
    target = jax.random.randint(key_target, (), 0, PEERS)
    peer_ids = jnp.arange(PEERS)
    counts = jnp.where(peer_ids[None, :] == full_peer[:, None], BLK, counts)
    counts = jnp.where(peer_ids[None, :] == target, BLK, counts)
    slots = jnp.arange(BLK)
    return jnp.where(slots[None, None, :] < counts[:, :, None], picked, -1).astype(jnp.int32)


def draw_tile_col(key, part):
    keys = jax.random.split(jax.random.fold_in(key, 21), PEERS)
    orders = jax.vmap(lambda single: jax.random.permutation(single, COL_BLOCKS))(keys)
    flat = jnp.arange(ROW_BLOCKS * TILES) % COL_BLOCKS
    picked = orders[:, flat]
    return picked.reshape(PEERS * ROW_BLOCKS, TILES).astype(jnp.int32)


def place_ends(drawn, stream_key, least, top_value):
    index_at = [jax.random.randint(jax.random.fold_in(stream_key, axis), (), 0, length) for axis, length in enumerate(drawn.shape)]
    main_axis = drawn.shape.index(max(drawn.shape))
    beside = index_at[:main_axis] + [(index_at[main_axis] + 1) % drawn.shape[main_axis]] + index_at[main_axis + 1:]
    return drawn.at[tuple(index_at)].set(least).at[tuple(beside)].set(top_value)


def levels(rng, dims, shards, low, largest):
    def one(position, blocks):
        draws = jax.random.uniform(jax.random.fold_in(jax.random.fold_in(rng, 6), position), (blocks,), jnp.float32, low / len(shards), largest / len(shards))
        return jnp.repeat(jnp.exp(draws), dims[position] // blocks).reshape((-1,) + (1,) * (len(dims) - position - 1))

    gain = one(*shards[0])
    for cut in shards[1:]:
        gain = gain * one(*cut)
    return gain


def centred(stream_key, extent, scale, reach, cuts=(), kind=jnp.bfloat16):
    drawn = scale * jax.random.normal(stream_key, extent, jnp.float32)
    if cuts:
        drawn = drawn * levels(stream_key, extent, cuts, -0.22, 0.18)
    return jnp.clip(drawn, -reach, reach).astype(kind)


def setup_inputs(seed: int = 0) -> dict:
    key_of = jax.random.split(jax.random.key(seed), 10)
    return {
        "features": centred(key_of[0], (VERTS, F_IN), 1.0, 6.0, ((0, 32),)),
        "w_inner": centred(key_of[1], (F_IN, HID), F_IN ** -0.5, 0.25),
        "bias_inner": centred(key_of[2], (HID,), 1.0, 6.0, (), jnp.float32),
        "w_outer": centred(key_of[3], (HID, CLASSES), HID ** -0.5, 0.375),
        "bias_outer": centred(key_of[4], (CLASSES,), 1.0, 6.0, (), jnp.float32),
        "tiles": centred(key_of[5], (PEERS * ROW_BLOCKS, TILES, BLK, BLK), (12.0 / (TILES * BLK) ** 0.5), 3.0, ((0, 32),)),
        "tile_col": draw_tile_col(jax.random.fold_in(key_of[9], 71), 0),
        "degrees": place_ends(jax.random.randint(key_of[7], (VERTS,), 1, 33), jax.random.fold_in(key_of[7], 1), 1, 32).astype(jnp.int32),
        "send_rows": draw_send_rows(jax.random.fold_in(key_of[9], 71), 0),
    }


def aggregate(feature_rows, tiles, tile_col, send_rows):
    width = feature_rows.shape[1]
    by_device = feature_rows.reshape(PEERS, V_DEV, width)
    tile_sets = tiles.reshape(PEERS, ROW_BLOCKS, TILES, BLK, BLK)
    col_sets = tile_col.reshape(PEERS, ROW_BLOCKS, TILES)

    def per_target(target):
        slot_rows = lax.dynamic_index_in_dim(send_rows, target, 1, keepdims=False)
        clipped = jnp.clip(slot_rows, 0, V_DEV - 1).astype(jnp.int32)
        fetched = jnp.take_along_axis(by_device, clipped[:, :, None], axis=1)
        fetched = jnp.where((slot_rows >= 0)[:, :, None], fetched, jnp.zeros((), feature_rows.dtype))
        own_rows = lax.dynamic_index_in_dim(by_device, target, 0, keepdims=False)
        columns = jnp.concatenate([own_rows.reshape(ROW_BLOCKS, BLK, width), fetched], axis=0)
        target_tiles = lax.dynamic_index_in_dim(tile_sets, target, 0, keepdims=False)
        target_cols = lax.dynamic_index_in_dim(col_sets, target, 0, keepdims=False)
        blocks = columns[target_cols]
        summed = jnp.einsum('rtij,rtjw->riw', target_tiles.astype(jnp.float32), blocks.astype(jnp.float32))
        return summed.reshape(V_DEV, width)
    results = lax.map(per_target, jnp.arange(PEERS, dtype=jnp.int32))
    return results.reshape(PEERS * V_DEV, width)

def reference(features, w_inner, bias_inner, w_outer, bias_outer, tiles, tile_col, degrees, send_rows):
    inv_sqrt = lax.rsqrt(degrees.astype(jnp.float32))[:, None]
    projected = (jnp.dot(features, w_inner, preferred_element_type=jnp.float32) * inv_sqrt).astype(jnp.bfloat16)
    agg_inner = aggregate(projected, tiles, tile_col, send_rows)
    hidden = (inv_sqrt * jax.nn.relu(inv_sqrt * agg_inner + bias_inner)).astype(jnp.bfloat16)
    scores = jnp.dot(hidden, w_outer, preferred_element_type=jnp.float32).astype(jnp.bfloat16)
    agg_outer = aggregate(scores, tiles, tile_col, send_rows)
    return inv_sqrt * agg_outer + bias_outer
```

```python
import functools

import jax
import jax.numpy as jnp
from jax import lax
from jax.experimental import pallas as pl
from jax.experimental.pallas import tpu as pltpu
from jax.sharding import PartitionSpec as P

MESH = pl.DeviceIdType.MESH
NT = (((1,), (1,)), ((), ()))
PARTS = 4
HALVES = 2


class Place:
    def __init__(self, n_dom, n_sub):
        self.n_dom, self.n_sub = n_dom, n_sub
        self.dom, self.sub = lax.axis_index("dom"), lax.axis_index("sub")
        self.mine = self.dom * n_sub + self.sub

    def flip(self, a):
        total, bit = 0, 1
        while bit < self.n_dom:
            total = total + lax.rem(lax.div(self.dom, bit) + lax.div(a, bit), 2) * bit
            bit *= 2
        return total

    def target(self, k):
        n_sub = self.n_sub
        return self.flip(lax.div(k, n_sub)), lax.rem(self.sub + lax.rem(k, n_sub), n_sub)

    def source(self, k):
        n_sub = self.n_sub
        return self.flip(lax.div(k, n_sub)) * n_sub + lax.rem(self.sub + n_sub - lax.rem(k, n_sub), n_sub)


def picked(first, second, table, lists):
    slots = jnp.concatenate([lists[pl.ds(first, 1), :], lists[pl.ds(second, 1), :]], axis=1)
    verts = table.shape[-1]
    hot = lax.broadcasted_iota(jnp.int32, (verts, slots.shape[1]), 0) == slots
    hot = jnp.where(hot, 1.0, 0.0).astype(table.dtype)
    return jnp.dot(table[...], hot, preferred_element_type=jnp.float32).astype(table.dtype)


def add(acc, block, c0, c1, fresh, tiles, where_tile):
    rows, _, blk, _ = tiles.shape

    def tile(r, c):
        t = where_tile[r, c]
        found = tiles[r, jnp.maximum(t, 0)]
        return jnp.where(t >= 0, found, jnp.zeros_like(found))

    for r in range(0, rows, 2):
        weights = jnp.concatenate(
            [jnp.concatenate([tile(r + q, c0), tile(r + q, c1)], axis=1) for q in range(2)], axis=0
        )
        term = lax.dot_general(block, weights, NT, preferred_element_type=jnp.float32)
        span = slice(r * blk, (r + 2) * blk)
        acc[:, span] = term if fresh else acc[:, span] + term


def prologue(place, hbm, staged, tiles_hbm, tiles, tile_sem, stage_sem, found, where_tile, found_sem, proj):
    ft, w_inner, _, _, degrees, _, tile_col = staged
    verts = proj.shape[1]
    part = verts // PARTS
    small = [
        pltpu.make_async_copy(src, dst, stage_sem.at[i])
        for i, (src, dst) in enumerate(zip(hbm, staged))
        if i
    ]
    wide = [
        pltpu.make_async_copy(
            hbm[0].at[:, pl.ds(v * part, part)], ft.at[:, pl.ds(v * part, part)], stage_sem.at[len(staged) + v]
        )
        for v in range(PARTS)
    ]
    small[0].start()
    small[3].start()
    for each in wide:
        each.start()
    for i in (1, 2, 4, 5):
        small[i].start()
    tile_copy = pltpu.make_async_copy(tiles_hbm, tiles, tile_sem)
    tile_copy.start()

    barrier = pltpu.get_barrier_semaphore()
    peers = place.n_dom * place.n_sub

    @pl.loop(1, peers)
    def _(k):
        pl.semaphore_signal(barrier, inc=1, device_id=place.target(k), device_id_type=MESH)

    small[0].wait()
    small[3].wait()
    inv = lax.rsqrt(degrees[...].astype(jnp.float32))
    w_t = w_inner[...].T
    for v in range(PARTS):
        span = slice(v * part, (v + 1) * part)
        wide[v].wait()
        term = jnp.dot(w_t, ft[:, span], preferred_element_type=jnp.float32)
        proj[:, span] = (term * inv[:, span]).astype(proj.dtype)
    for i in (1, 2, 4, 5):
        small[i].wait()
    cols = tile_col[...]
    lane = lax.broadcasted_iota(jnp.int32, found.shape, 1)
    at = jnp.full(found.shape, -1, jnp.int32)
    for t in range(cols.shape[1]):
        at = jnp.where(cols[:, t:t + 1] == lane, t, at)
    found[...] = at
    found_copy = pltpu.make_async_copy(found, where_tile, found_sem)
    found_copy.start()
    pl.semaphore_wait(barrier, peers - 1)
    return inv, tile_copy, found_copy


def score(acc_in, inv, bias_col, w_pad, scores, blk):
    for v in range(0, scores.shape[1], blk):
        span = slice(v, v + blk)
        scale = inv[:, span]
        hidden = scale * jnp.maximum(scale * acc_in[:, span] + bias_col, 0.0)
        scores[:, span] = jnp.dot(
            w_pad[...], hidden.astype(jnp.bfloat16), preferred_element_type=jnp.float32
        ).astype(scores.dtype)


def relay_kernel(n_dom, n_sub, *refs):
    hbm, (tiles_hbm, out), staged, refs = refs[:7], refs[7:9], refs[9:16], refs[16:]
    (
        stage_sem, found, where_tile, found_sem, proj, out_in, got_in, acc_in, w_pad, scores, out_sc, got_sc,
        acc_sc, tiles, tile_sem, send_in, recv_in, send_sc, recv_sc, far_proj, far_lists, proj_send, proj_recv,
        lists_send, lists_recv,
    ) = refs
    _, _, bias, w_outer, _, lists, _ = staged
    place = Place(n_dom, n_sub)
    dom, sub, mine, flip = place.dom, place.sub, place.mine, place.flip
    hid, verts = proj.shape
    blk = tiles.shape[2]
    own = verts // blk
    classes = w_outer.shape[0]
    part = hid // HALVES
    per_step = 2 * n_dom
    half = lax.div(sub, 2)
    sibling, near, far = 1 + 4 * half - sub, 2 - half, 3 - 3 * half
    mid = lax.rem(sub + half, 2)
    middle = mid == 1
    edge = mid == 0

    inv, tile_copy, found_copy = prologue(
        place, hbm, staged, tiles_hbm, tiles, tile_sem, stage_sem, found, where_tile, found_sem, proj
    )

    def lists_copy(slot):
        return pltpu.make_async_remote_copy(
            src_ref=lists, dst_ref=far_lists.at[slot], send_sem=lists_send, recv_sem=lists_recv.at[slot],
            device_id=(dom, near), device_id_type=MESH,
        )

    def piece_copy(slot, c):
        rows = pl.ds(c * part, part)
        return pltpu.make_async_remote_copy(
            src_ref=proj.at[rows], dst_ref=far_proj.at[slot, rows], send_sem=proj_send.at[c],
            recv_sem=proj_recv.at[slot, c], device_id=(dom, near), device_id_type=MESH,
        )

    def send_table(slot):
        lists_copy(slot).start()
        for c in range(HALVES):
            piece_copy(slot, c).start()

    def list_copy(j, e, to_dom, to_sub):
        return pltpu.make_async_remote_copy(
            src_ref=out_in.at[j], dst_ref=got_in.at[e], send_sem=send_in.at[j], recv_sem=recv_in.at[0, e],
            device_id=(to_dom, to_sub), device_id_type=MESH,
        )

    def half_copy(j, e, c, to_dom, to_sub):
        rows = pl.ds(c * part, part)
        return pltpu.make_async_remote_copy(
            src_ref=out_in.at[j, rows], dst_ref=got_in.at[e, rows], send_sem=send_in.at[j],
            recv_sem=recv_in.at[c, e], device_id=(to_dom, to_sub), device_id_type=MESH,
        )

    def hand_out_own():
        def pair(a):
            row = flip(a) * n_sub
            return picked(row + sub, row + sibling, proj, lists)

        first = pair(0)
        got_in[mine] = first[:, :blk]
        out_in[1] = first[:, blk:]
        list_copy(1, mine, dom, sibling).start()

        @pl.loop(1, n_dom)
        def _(a):
            both = pair(a)
            j = 2 * a
            out_in[j] = both[:, :blk]
            out_in[j + 1] = both[:, blk:]
            list_copy(j + 1, mine, flip(a), sibling).start()
            list_copy(j, mine, flip(a), sub).start()

    def relay(slot, c, from_sub):
        if c == 0:
            lists_copy(slot).wait_recv()
        piece_copy(slot, c).wait_recv()
        e = dom * n_sub + from_sub
        base = (slot + 1) * per_step
        rows = slice(c * part, (c + 1) * part)

        def pair(a):
            row = flip(a) * n_sub
            return picked(row + sub, row + sibling, far_proj.at[slot, rows], far_lists.at[slot])

        first = pair(0)
        got_in[e, rows, :] = first[:, :blk]
        out_in[base + 1, rows, :] = first[:, blk:]
        half_copy(base + 1, e, c, dom, sibling).start()

        @pl.loop(1, n_dom)
        def _(a):
            both = pair(a)
            j = base + 2 * a
            out_in[j, rows, :] = both[:, :blk]
            out_in[j + 1, rows, :] = both[:, blk:]
            half_copy(j + 1, e, c, flip(a), sibling).start()
            half_copy(j, e, c, flip(a), sub).start()

    def add_own(table, acc):
        for c in range(0, own, 2):
            add(acc, table[:, c * blk:(c + 2) * blk], c, c + 1, c == 0, tiles, where_tile)

    def pair_of(m, plane):
        return flip(2 * m) * n_sub + plane, flip(2 * m + 1) * n_sub + plane

    def add_whole(m, plane):
        e0, e1 = pair_of(m, plane)
        add(
            acc_in, jnp.concatenate([got_in[e0], got_in[e1]], axis=1), own + e0, own + e1, False, tiles, where_tile
        )

    def add_plane(plane):
        for i, e in enumerate(pair_of(0, plane)):
            if i:
                list_copy(0, e, dom, sibling).wait_recv()
            else:
                @pl.when(plane != sub)
                def _():
                    list_copy(0, e, dom, sibling).wait_recv()
        add_whole(0, plane)

        @pl.loop(1, n_dom // 2)
        def _(m):
            for e in pair_of(m, plane):
                list_copy(0, e, dom, sibling).wait_recv()
            add_whole(m, plane)

    def await_pair(m, plane, c):
        for e in pair_of(m, plane):
            half_copy(0, e, c, dom, sibling).wait_recv()

    def add_relayed(plane):
        _, e1 = pair_of(0, plane)
        for c in range(HALVES):
            half_copy(0, e1, c, dom, sibling).wait_recv()
        add_whole(0, plane)

        @pl.loop(1, n_dom // 2)
        def _(m):
            for c in range(HALVES):
                await_pair(m, plane, c)
            add_whole(m, plane)

    def add_halves(plane, c):
        rows = slice(c * part, (c + 1) * part)

        @pl.loop(0, n_dom // 2)
        def _(m):
            e0, e1 = pair_of(m, plane)
            await_pair(m, plane, c)
            block = jnp.concatenate([got_in[e0, rows, :], got_in[e1, rows, :]], axis=1)
            add(acc_in.at[rows], block, own + e0, own + e1, False, tiles, where_tile)

    pl.when(middle)(lambda: send_table(0))
    hand_out_own()
    pl.when(edge)(lambda: send_table(1))
    w_pad[...] = jnp.zeros_like(w_pad)
    w_pad[0:classes, :] = w_outer[...]
    bias_col = jnp.broadcast_to(bias[...], (blk, hid)).T
    tile_copy.wait()
    found_copy.wait()
    add_own(proj, acc_in)
    add_plane(sub)

    @pl.when(middle)
    def _():
        relay(0, 0, near)
        relay(0, 1, near)
        add_plane(sibling)
        relay(1, 0, far)
        add_relayed(near)
        relay(1, 1, far)
        add_relayed(far)

    @pl.when(edge)
    def _():
        add_plane(sibling)
        for plane in (near, far):
            for c in range(HALVES):
                add_halves(plane, c)

    score(acc_in, inv, bias_col, w_pad, scores, blk)

    def score_copy(k, e, to_dom, to_sub):
        return pltpu.make_async_remote_copy(
            src_ref=out_sc.at[k], dst_ref=got_sc.at[e], send_sem=send_sc.at[k], recv_sem=recv_sc.at[e],
            device_id=(to_dom, to_sub), device_id_type=MESH,
        )

    def deliver(i, plane, last):
        def send(m):
            both = picked(*pair_of(m, plane), scores, lists)
            for q in range(2):
                k = i * n_dom + 2 * m + q
                out_sc[k] = both[:, q * blk:(q + 1) * blk]
                score_copy(k, mine, flip(2 * m + q), plane).start()

        @pl.loop(0, n_dom // 2 - last)
        def _(m):
            send(n_dom // 2 - 1 - m)

        if last:
            both = picked(*pair_of(0, plane), scores, lists)
            got_sc[mine] = both[:, :blk]
            out_sc[i * n_dom + 1] = both[:, blk:]
            score_copy(i * n_dom + 1, mine, flip(1), plane).start()

    def add_scores(m, plane):
        e0, e1 = pair_of(m, plane)
        block = jnp.concatenate([got_sc[e0], got_sc[e1]], axis=1)
        add(acc_sc, block, own + e0, own + e1, False, tiles, where_tile)

    def gather(plane):
        @pl.loop(0, n_dom // 2 - 1)
        def _(i):
            m = n_dom // 2 - 1 - i
            for e in pair_of(m, plane):
                score_copy(0, e, dom, sibling).wait_recv()
            add_scores(m, plane)

        e0, e1 = pair_of(0, plane)

        @pl.when(plane != sub)
        def _():
            score_copy(0, e0, dom, sibling).wait_recv()

        score_copy(0, e1, dom, sibling).wait_recv()
        add_scores(0, plane)

    for i, plane in enumerate((far, near, sibling, sub)):
        deliver(i, plane, int(i == 3))
    add_own(scores, acc_sc)

    @pl.loop(1, per_step)
    def _(j):
        list_copy(j, 0, dom, sibling).wait_send()

    lists_copy(0).wait_send()
    for c in range(HALVES):
        piece_copy(0, c).wait_send()

    @pl.when(middle)
    def _():
        for base in (per_step, 2 * per_step):
            @pl.loop(1, per_step)
            def _(j):
                list_copy(base + j, 0, dom, sibling).wait_send()

    gather(sibling + mid * (sub - sibling))
    gather(near)
    gather(sub + mid * (sibling - sub))

    @pl.loop(0, n_dom * n_sub)
    def _(k):
        @pl.when(k != 3 * n_dom)
        def _():
            score_copy(k, 0, dom, sibling).wait_send()

    gather(far)
    out[...] = inv * acc_sc[0:classes, :]


def direct_kernel(n_dom, n_sub, *refs):
    hbm, (tiles_hbm, out), staged, refs = refs[:7], refs[7:9], refs[9:16], refs[16:]
    (
        stage_sem, found, where_tile, found_sem, proj, out_in, got_in, acc_in, w_pad, scores, out_sc, got_sc,
        acc_sc, tiles, tile_sem, send_in, recv_in, send_sc, recv_sc,
    ) = refs
    _, _, bias, w_outer, _, lists, _ = staged
    place = Place(n_dom, n_sub)
    peers = n_dom * n_sub
    hid, verts = proj.shape
    blk = tiles.shape[2]
    own = verts // blk
    classes = w_outer.shape[0]

    inv, tile_copy, found_copy = prologue(
        place, hbm, staged, tiles_hbm, tiles, tile_sem, stage_sem, found, where_tile, found_sem, proj
    )

    def copy(src, dst, sends, recvs, k):
        return pltpu.make_async_remote_copy(
            src_ref=src.at[k], dst_ref=dst.at[k], send_sem=sends.at[k], recv_sem=recvs.at[k],
            device_id=place.target(k), device_id_type=MESH,
        )

    def pick(k, table):
        index = [to_dom * n_sub + to_sub for to_dom, to_sub in (place.target(k), place.target(k + 1))]
        return picked(*index, table, lists)

    def deliver(table, outgoing, got, sends, recvs):
        first = pick(0, table)
        got[0] = first[:, :blk]
        outgoing[1] = first[:, blk:]
        copy(outgoing, got, sends, recvs, 1).start()

        @pl.loop(1, peers // 2)
        def _(pair):
            k = 2 * pair
            both = pick(k, table)
            outgoing[k] = both[:, :blk]
            outgoing[k + 1] = both[:, blk:]
            copy(outgoing, got, sends, recvs, k).start()
            copy(outgoing, got, sends, recvs, k + 1).start()

    def aggregate(table, outgoing, got, sends, recvs, acc):
        for c in range(0, own, 2):
            add(acc, table[:, c * blk:(c + 2) * blk], c, c + 1, c == 0, tiles, where_tile)

        def arrived(k):
            block = jnp.concatenate([got[k], got[k + 1]], axis=1)
            add(acc, block, own + place.source(k), own + place.source(k + 1), False, tiles, where_tile)

        copy(outgoing, got, sends, recvs, 1).wait_recv()
        arrived(0)

        @pl.loop(1, peers // 2)
        def _(pair):
            k = 2 * pair
            copy(outgoing, got, sends, recvs, k).wait_recv()
            copy(outgoing, got, sends, recvs, k + 1).wait_recv()
            arrived(k)

    deliver(proj, out_in, got_in, send_in, recv_in)
    w_pad[...] = jnp.zeros_like(w_pad)
    w_pad[0:classes, :] = w_outer[...]
    bias_col = jnp.broadcast_to(bias[...], (blk, hid)).T
    tile_copy.wait()
    found_copy.wait()
    aggregate(proj, out_in, got_in, send_in, recv_in, acc_in)
    score(acc_in, inv, bias_col, w_pad, scores, blk)
    deliver(scores, out_sc, got_sc, send_sc, recv_sc)
    aggregate(scores, out_sc, got_sc, send_sc, recv_sc, acc_sc)
    out[...] = inv * acc_sc[0:classes, :]

    @pl.loop(1, peers)
    def _(k):
        copy(out_in, got_in, send_in, recv_in, k).wait_send()
        copy(out_sc, got_sc, send_sc, recv_sc, k).wait_send()


def on_device(
    n_dom, n_sub,
    features, w_inner, bias_inner, w_outer, bias_outer, tiles, tile_col, degrees, send_rows
):
    peers = n_dom * n_sub
    verts, hid = features.shape[0], w_inner.shape[1]
    classes = w_outer.shape[1]
    padded = 16 * ((classes + 15) // 16)
    blk = tiles.shape[2]
    columns = verts // blk + peers
    lanes = 128 * ((columns + 127) // 128)
    small = (
        features.T, w_inner, bias_inner[None, :], w_outer.T, degrees[None, :], send_rows[0], tile_col
    )
    relay = n_sub == 4
    lists_out = 6 * n_dom if relay else peers
    vmem = pl.BlockSpec(memory_space=pltpu.VMEM)
    bf16, f32 = jnp.bfloat16, jnp.float32
    agg = pl.pallas_call(
        functools.partial(relay_kernel if relay else direct_kernel, n_dom, n_sub),
        out_shape=jax.ShapeDtypeStruct((classes, verts), f32),
        in_specs=[pl.BlockSpec(memory_space=pl.ANY)] * 8,
        out_specs=vmem,
        scratch_shapes=[pltpu.VMEM(each.shape, each.dtype) for each in small]
        + [
            pltpu.SemaphoreType.DMA((len(small) + PARTS,)),
            pltpu.VMEM((tiles.shape[0], lanes), jnp.int32),
            pltpu.SMEM((tiles.shape[0], lanes), jnp.int32),
            pltpu.SemaphoreType.DMA,
            pltpu.VMEM((hid, verts), bf16),
            pltpu.VMEM((lists_out, hid, blk), bf16),
            pltpu.VMEM((peers, hid, blk), bf16),
            pltpu.VMEM((hid, verts), f32),
            pltpu.VMEM((padded, hid), bf16),
            pltpu.VMEM((padded, verts), bf16),
            pltpu.VMEM((peers, padded, blk), bf16),
            pltpu.VMEM((peers, padded, blk), bf16),
            pltpu.VMEM((padded, verts), f32),
            pltpu.VMEM(tiles.shape, bf16),
            pltpu.SemaphoreType.DMA,
            pltpu.SemaphoreType.DMA((lists_out,)),
            pltpu.SemaphoreType.DMA((HALVES, peers) if relay else (peers,)),
            pltpu.SemaphoreType.DMA((peers,)),
            pltpu.SemaphoreType.DMA((peers,)),
        ]
        + (
            [
                pltpu.VMEM((2, hid, verts), bf16),
                pltpu.VMEM((2, peers, blk), jnp.int32),
                pltpu.SemaphoreType.DMA((HALVES,)),
                pltpu.SemaphoreType.DMA((2, HALVES)),
                pltpu.SemaphoreType.DMA,
                pltpu.SemaphoreType.DMA((2,)),
            ]
            if relay
            else []
        ),
        compiler_params=pltpu.CompilerParams(
            collective_id=0, has_side_effects=True, vmem_limit_bytes=56 * 1024 * 1024
        ),
    )(*small, tiles)
    return agg.T + bias_outer


def solution(mesh):
    return jax.shard_map(
        functools.partial(on_device, mesh.shape["dom"], mesh.shape["sub"]),
        mesh=mesh,
        in_specs=(
            P(("dom", "sub"), None),
            P(),
            P(),
            P(),
            P(),
            P(("dom", "sub"), None, None, None),
            P(("dom", "sub"), None),
            P(("dom", "sub")),
            P(("dom", "sub"), None, None),
        ),
        out_specs=P(("dom", "sub"), None),
        check_vma=False,
    )
```

```python
import functools

import jax
import jax.numpy as jnp
from jax import lax
from jax.experimental import pallas as pl
from jax.experimental.pallas import tpu as pltpu
from jax.sharding import PartitionSpec as P

MESH = pl.DeviceIdType.MESH
NT = (((1,), (1,)), ((), ()))
PARTS = 4
HALVES = 2


class Place:
    def __init__(self, n_dom, n_sub):
        self.n_dom, self.n_sub = n_dom, n_sub
        self.dom, self.sub = lax.axis_index("dom"), lax.axis_index("sub")
        self.mine = self.dom * n_sub + self.sub

    def flip(self, a):
        total, bit = 0, 1
        while bit < self.n_dom:
            total = total + lax.rem(lax.div(self.dom, bit) + lax.div(a, bit), 2) * bit
            bit *= 2
        return total

    def target(self, k):
        n_sub = self.n_sub
        return self.flip(lax.div(k, n_sub)), lax.rem(self.sub + lax.rem(k, n_sub), n_sub)

    def source(self, k):
        n_sub = self.n_sub
        return self.flip(lax.div(k, n_sub)) * n_sub + lax.rem(self.sub + n_sub - lax.rem(k, n_sub), n_sub)


def hot_of(first, second, lists, verts):
    slots = jnp.concatenate([lists[pl.ds(first, 1), :], lists[pl.ds(second, 1), :]], axis=1)
    hot = lax.broadcasted_iota(jnp.int32, (verts, slots.shape[1]), 0) == slots
    return jnp.where(hot, 1.0, 0.0).astype(jnp.bfloat16)


def taken(table, hot):
    return jnp.dot(table[...], hot, preferred_element_type=jnp.float32).astype(table.dtype)


def picked(first, second, table, lists):
    return taken(table, hot_of(first, second, lists, table.shape[-1]))


def add(acc, block, c0, c1, fresh, tiles, where_tile):
    rows, _, blk, _ = tiles.shape

    def tile(r, c):
        t = where_tile[r, c]
        found = tiles[r, jnp.maximum(t, 0)]
        return jnp.where(t >= 0, found, jnp.zeros_like(found))

    for r in range(0, rows, 2):
        weights = jnp.concatenate(
            [jnp.concatenate([tile(r + q, c0), tile(r + q, c1)], axis=1) for q in range(2)], axis=0
        )
        term = lax.dot_general(block, weights, NT, preferred_element_type=jnp.float32)
        span = slice(r * blk, (r + 2) * blk)
        acc[:, span] = term if fresh else acc[:, span] + term


def prologue(place, hbm, staged, tiles_hbm, tiles, tile_sem, stage_sem, found, where_tile, found_sem, proj, greet):
    ft, w_inner, _, _, degrees, _, tile_col = staged
    verts = proj.shape[1]
    part = verts // PARTS
    small = [
        pltpu.make_async_copy(src, dst, stage_sem.at[i])
        for i, (src, dst) in enumerate(zip(hbm, staged))
        if i
    ]
    wide = [
        pltpu.make_async_copy(
            hbm[0].at[:, pl.ds(v * part, part)], ft.at[:, pl.ds(v * part, part)], stage_sem.at[len(staged) + v]
        )
        for v in range(PARTS)
    ]
    small[0].start()
    small[3].start()
    for each in wide:
        each.start()
    for i in (1, 2, 4, 5):
        small[i].start()
    tile_copy = pltpu.make_async_copy(tiles_hbm, tiles, tile_sem)

    greet()

    small[0].wait()
    small[3].wait()
    inv = lax.rsqrt(degrees[...].astype(jnp.float32))
    w_t = w_inner[...].T
    for v in range(PARTS):
        span = slice(v * part, (v + 1) * part)
        wide[v].wait()
        term = jnp.dot(w_t, ft[:, span], preferred_element_type=jnp.float32)
        if v == PARTS - 1:
            tile_copy.start()
        proj[:, span] = (term * inv[:, span]).astype(proj.dtype)
    for i in (1, 2, 4, 5):
        small[i].wait()
    cols = tile_col[...]
    lane = lax.broadcasted_iota(jnp.int32, found.shape, 1)
    at = jnp.full(found.shape, -1, jnp.int32)
    for t in range(cols.shape[1]):
        at = jnp.where(cols[:, t:t + 1] == lane, t, at)
    found[...] = at
    found_copy = pltpu.make_async_copy(found, where_tile, found_sem)
    found_copy.start()
    return inv, tile_copy, found_copy


def turn_of(i, count):
    return count - 1 - lax.div(i, 2) - count // 2 * lax.rem(i, 2)


def score(acc_in, inv, bias_col, w_pad, scores, blk):
    for v in range(0, scores.shape[1], blk):
        span = slice(v, v + blk)
        scale = inv[:, span]
        hidden = scale * jnp.maximum(scale * acc_in[:, span] + bias_col, 0.0)
        scores[:, span] = jnp.dot(
            w_pad[...], hidden.astype(jnp.bfloat16), preferred_element_type=jnp.float32
        ).astype(scores.dtype)


def relay_kernel(n_dom, n_sub, *refs):
    hbm, (tiles_hbm, out), staged, refs = refs[:7], refs[7:9], refs[9:16], refs[16:]
    (
        stage_sem, found, where_tile, found_sem, proj, out_in, got_in, acc_in, w_pad, scores, out_sc, got_sc,
        acc_sc, tiles, tile_sem, send_in, recv_in, send_sc, recv_sc, far_proj, far_lists, proj_send, proj_recv,
        lists_send, lists_recv, dense, hots, clear,
    ) = refs
    _, _, bias, w_outer, _, lists, _ = staged
    place = Place(n_dom, n_sub)
    dom, sub, flip = place.dom, place.sub, place.flip
    hid, verts = proj.shape
    blk = tiles.shape[2]
    own = verts // blk
    classes = w_outer.shape[0]
    part = hid // HALVES
    pairs = n_dom // 2
    per_step = 2 * n_dom
    peers = n_dom * n_sub
    half = lax.div(sub, 2)
    sibling, near, far = 1 + 4 * half - sub, 2 - half, 3 - 3 * half
    mid = lax.rem(sub + half, 2)
    middle, edge = mid == 1, mid == 0
    barrier = pltpu.get_barrier_semaphore()

    def greet():
        @pl.loop(1, peers)
        def _(k):
            pl.semaphore_signal(barrier, inc=1, device_id=place.target(k), device_id_type=MESH)

    inv, tile_copy, found_copy = prologue(
        place, hbm, staged, tiles_hbm, tiles, tile_sem, stage_sem, found, where_tile, found_sem, proj, greet
    )

    def lists_copy(slot):
        return pltpu.make_async_remote_copy(
            src_ref=lists, dst_ref=far_lists.at[slot], send_sem=lists_send, recv_sem=lists_recv.at[slot],
            device_id=(dom, near), device_id_type=MESH,
        )

    def piece_copy(slot, c):
        rows = pl.ds(c * part, part)
        return pltpu.make_async_remote_copy(
            src_ref=proj.at[rows], dst_ref=far_proj.at[slot, rows], send_sem=proj_send,
            recv_sem=proj_recv.at[slot, c], device_id=(dom, near), device_id_type=MESH,
        )

    def send_table(slot):
        lists_copy(slot).start()
        for c in range(HALVES):
            piece_copy(slot, c).start()

    def await_table():
        lists_copy(0).wait_send()
        pltpu.make_async_remote_copy(
            src_ref=proj, dst_ref=far_proj.at[0], send_sem=proj_send, recv_sem=proj_recv.at[0, 0],
            device_id=(dom, near), device_id_type=MESH,
        ).wait_send()

    def came_in(plane, m, c):
        return recv_in.at[(n_sub * pairs + lax.rem(plane, 2) * pairs if c else plane * pairs) + m]

    def lists_of(ref, at, c):
        return ref.at[at] if c is None else ref.at[at, pl.ds(c * part, part)]

    def list_copy(j, plane, a, c, to_sub, relayed):
        return pltpu.make_async_remote_copy(
            src_ref=lists_of(out_in, j, c), dst_ref=lists_of(got_in, plane * n_dom + a, c),
            send_sem=send_in.at[relayed], recv_sem=came_in(plane, lax.div(a, 2), c),
            device_id=(flip(a), to_sub), device_id_type=MESH,
        )

    def await_lists(plane, m, c, count=2):
        at = pl.ds(plane * n_dom + 2 * m + 2 - count, count)
        pltpu.make_async_remote_copy(
            src_ref=lists_of(out_in, pl.ds(0, count), c), dst_ref=lists_of(got_in, at, c),
            send_sem=send_in.at[0], recv_sem=came_in(plane, m, c),
            device_id=(dom, sibling), device_id_type=MESH,
        ).wait_recv()

    def await_sent(relayed, count):
        pltpu.make_async_remote_copy(
            src_ref=out_in.at[pl.ds(0, count)], dst_ref=out_in.at[pl.ds(0, count)],
            send_sem=send_in.at[relayed], recv_sem=recv_in.at[0],
            device_id=(dom, sibling), device_id_type=MESH,
        ).wait_send()

    def keep_hot(a, hot, first, second):
        at = pl.ds(pl.multiple_of(a * blk, blk), blk)
        hots[first, :, at] = hot[:, :blk]
        hots[second, :, at] = hot[:, blk:]

    def pick_own(a):
        row = flip(a) * n_sub
        hot = hot_of(row + sub, row + sibling, lists, verts)
        keep_hot(a, hot, sub, sibling)
        both = taken(proj, hot)
        out_in[2 * a + 1] = both[:, blk:]
        return both[:, :blk]

    def pick_both(a):
        out_in[2 * a] = pick_own(a)

    def send_both(a):
        list_copy(2 * a + 1, sub, a, None, sibling, 0).start()
        list_copy(2 * a, sub, a, None, sub, 0).start()

    def hand_out_own():
        send_both(n_dom - 1)

        @pl.loop(1, n_dom - 1)
        def _(i):
            pick_both(turn_of(i, n_dom))
            send_both(turn_of(i, n_dom))

        got_in[sub * n_dom] = pick_own(0)
        list_copy(1, sub, 0, None, sibling, 0).start()

    def turn(begin, end, column_of, at):
        def tile(r, c):
            t = where_tile[r, c]
            found = tiles[r, jnp.maximum(t, 0)]
            return jnp.where(t >= 0, found, jnp.zeros_like(found))

        @pl.loop(begin, end)
        def _(i):
            c = column_of(i)
            for r in range(0, tiles.shape[0], 2):
                both = jnp.concatenate([tile(r, c), tile(r + 1, c)], axis=0)
                dense[at + i, :, r * blk:(r + 2) * blk] = both.T

    def turn_slots(begin, end):
        turn(begin, end, lambda i: own + flip(lax.rem(i, n_dom)) * n_sub + lax.div(i, n_dom), own)

    def keep_far_hots():
        @pl.loop(0, n_dom)
        def _(a):
            row = flip(a) * n_sub
            keep_hot(a, hot_of(row + near, row + far, lists, verts), near, far)

    def relay(slot, c, plane):
        if c == 0:
            lists_copy(slot).wait_recv()
        piece_copy(slot, c).wait_recv()
        base = (slot + 1) * per_step
        rows = slice(c * part, (c + 1) * part)

        def pair(a):
            row = flip(a) * n_sub
            return picked(row + sub, row + sibling, far_proj.at[slot, rows], far_lists.at[slot])

        @pl.loop(0, n_dom - 1)
        def _(i):
            a = turn_of(i, n_dom)
            both = pair(a)
            j = base + 2 * a
            out_in[j, rows, :] = both[:, :blk]
            out_in[j + 1, rows, :] = both[:, blk:]
            list_copy(j + 1, plane, a, c, sibling, 1).start()
            list_copy(j, plane, a, c, sub, 1).start()

        first = pair(0)
        got_in[plane * n_dom, rows, :] = first[:, :blk]
        out_in[base + 1, rows, :] = first[:, blk:]
        list_copy(base + 1, plane, 0, c, sibling, 1).start()

    wide = 2 * blk

    def add_dense(acc, block, first, count, fresh):
        for v in range(0, verts, wide):
            span = slice(v, v + wide)
            weights = dense[pl.ds(first, count), :, span].reshape(count * blk, wide)
            term = jnp.dot(block, weights, preferred_element_type=jnp.float32)
            acc[:, span] = term if fresh else acc[:, span] + term

    def add_own(table, acc):
        add_dense(acc, table[...], 0, own, True)

    def add_pair(plane, m):
        slot = plane * n_dom + 2 * m
        add_dense(acc_in, jnp.concatenate([got_in[slot], got_in[slot + 1]], axis=1), own + slot, 2, False)

    def add_plane(plane, halves, local):
        parts = range(HALVES) if halves else (None,)

        @pl.loop(0, pairs - 1)
        def _(i):
            m = turn_of(i, pairs)
            for c in parts:
                await_lists(plane, m, c)
            add_pair(plane, m)

        for c in parts:
            await_lists(plane, 0, c, 1 if local else 2)
        add_pair(plane, 0)

    def add_halves(plane, c):
        rows = slice(c * part, (c + 1) * part)

        @pl.loop(0, pairs)
        def _(i):
            m = turn_of(i, pairs)
            slot = plane * n_dom + 2 * m
            await_lists(plane, m, c)
            block = jnp.concatenate([got_in[slot, rows, :], got_in[slot + 1, rows, :]], axis=1)
            add_dense(acc_in.at[rows], block, own + slot, 2, False)

    pick_both(n_dom - 1)
    pl.semaphore_wait(barrier, peers - 1)
    pl.when(middle)(lambda: send_table(0))
    hand_out_own()
    w_pad[...] = jnp.zeros_like(w_pad)
    w_pad[0:classes, :] = w_outer[...]
    bias_col = jnp.broadcast_to(bias[...], (blk, hid)).T
    tile_copy.wait()
    found_copy.wait()
    turn(0, own, lambda i: i, 0)
    turn_slots(0, n_dom)
    keep_far_hots()

    @pl.when(middle)
    def _():
        relay(0, 0, near)
        turn_slots(n_dom, 2 * n_dom)
        await_table()
        pl.semaphore_signal(clear, inc=1, device_id=(dom, sibling), device_id_type=MESH)
        turn_slots(2 * n_dom, peers)
        relay(0, 1, near)
        add_own(proj, acc_in)
        add_plane(sub, False, True)
        relay(1, 0, far)
        add_plane(sibling, False, False)
        relay(1, 1, far)
        add_plane(near, True, True)
        add_plane(far, True, True)

    @pl.when(edge)
    def _():
        turn_slots(n_dom, peers)
        add_own(proj, acc_in)
        pl.semaphore_wait(clear, 1)
        send_table(1)
        add_plane(sub, False, True)
        add_plane(sibling, False, False)
        add_halves(near, 0)
        add_halves(near, 1)
        add_halves(far, 0)
        add_halves(far, 1)

    score(acc_in, inv, bias_col, w_pad, scores, blk)

    def score_copy(k, a, plane):
        return pltpu.make_async_remote_copy(
            src_ref=out_sc.at[k], dst_ref=got_sc.at[sub * n_dom + a], send_sem=send_sc, recv_sem=recv_sc.at[sub],
            device_id=(flip(a), plane), device_id_type=MESH,
        )

    def deliver(plane):
        lists_for = taken(scores, hots[plane])
        for a in [n_dom - 1 - i // 2 - n_dom // 2 * (i % 2) for i in range(n_dom)]:
            k = plane * n_dom + a
            out_sc[k] = lists_for[:, a * blk:(a + 1) * blk]
            if a:
                score_copy(k, a, plane).start()
            else:
                pl.when(sub != plane)(lambda: score_copy(k, 0, plane).start())

        @pl.when(sub == plane)
        def _():
            got_sc[sub * n_dom] = lists_for[:, :blk]

    def scores_wait(at, count, plane):
        return pltpu.make_async_remote_copy(
            src_ref=out_sc.at[pl.ds(0, count)], dst_ref=got_sc.at[pl.ds(at, count)], send_sem=send_sc,
            recv_sem=recv_sc.at[plane], device_id=(dom, sibling), device_id_type=MESH,
        )

    def gather(plane):
        slot = plane * n_dom
        pl.when(plane != sub)(lambda: scores_wait(slot, n_dom, plane).wait_recv())
        pl.when(plane == sub)(lambda: scores_wait(slot + 1, n_dom - 1, plane).wait_recv())
        block = jnp.concatenate([got_sc[slot + a] for a in range(n_dom)], axis=1)
        add_dense(acc_sc, block, own + slot, n_dom, False)

    @pl.when(middle)
    def _():
        for plane in (sub, near, sibling):
            deliver(plane)
        await_sent(1, 2 * (per_step - 1))
        deliver(far)

    @pl.when(edge)
    def _():
        for plane in (far, sub, near, sibling):
            deliver(plane)

    add_own(scores, acc_sc)
    await_sent(0, per_step - 1)
    pl.when(edge)(await_table)
    gather(sibling + mid * (sub - sibling))
    gather(near)
    gather(sub + mid * (sibling - sub))
    gather(far)
    out[...] = inv * acc_sc[0:classes, :]
    scores_wait(0, peers - 1, 0).wait_send()


def direct_kernel(n_dom, n_sub, *refs):
    hbm, (tiles_hbm, out), staged, refs = refs[:7], refs[7:9], refs[9:16], refs[16:]
    (
        stage_sem, found, where_tile, found_sem, proj, out_in, got_in, acc_in, w_pad, scores, out_sc, got_sc,
        acc_sc, tiles, tile_sem, send_in, recv_in, send_sc, recv_sc,
    ) = refs
    _, _, bias, w_outer, _, lists, _ = staged
    place = Place(n_dom, n_sub)
    peers = n_dom * n_sub
    hid, verts = proj.shape
    blk = tiles.shape[2]
    own = verts // blk
    classes = w_outer.shape[0]

    barrier = pltpu.get_barrier_semaphore()

    def greet():
        @pl.loop(1, peers)
        def _(k):
            pl.semaphore_signal(barrier, inc=1, device_id=place.target(k), device_id_type=MESH)

    inv, tile_copy, found_copy = prologue(
        place, hbm, staged, tiles_hbm, tiles, tile_sem, stage_sem, found, where_tile, found_sem, proj, greet
    )
    pl.semaphore_wait(barrier, peers - 1)

    def copy(src, dst, sends, recvs, k):
        return pltpu.make_async_remote_copy(
            src_ref=src.at[k], dst_ref=dst.at[k], send_sem=sends.at[k], recv_sem=recvs.at[k],
            device_id=place.target(k), device_id_type=MESH,
        )

    def pick(k, table):
        index = [to_dom * n_sub + to_sub for to_dom, to_sub in (place.target(k), place.target(k + 1))]
        return picked(*index, table, lists)

    def deliver(table, outgoing, got, sends, recvs):
        first = pick(0, table)
        got[0] = first[:, :blk]
        outgoing[1] = first[:, blk:]
        copy(outgoing, got, sends, recvs, 1).start()

        @pl.loop(1, peers // 2)
        def _(pair):
            k = 2 * pair
            both = pick(k, table)
            outgoing[k] = both[:, :blk]
            outgoing[k + 1] = both[:, blk:]
            copy(outgoing, got, sends, recvs, k).start()
            copy(outgoing, got, sends, recvs, k + 1).start()

    def aggregate(table, outgoing, got, sends, recvs, acc):
        for c in range(0, own, 2):
            add(acc, table[:, c * blk:(c + 2) * blk], c, c + 1, c == 0, tiles, where_tile)

        def arrived(k):
            block = jnp.concatenate([got[k], got[k + 1]], axis=1)
            add(acc, block, own + place.source(k), own + place.source(k + 1), False, tiles, where_tile)

        copy(outgoing, got, sends, recvs, 1).wait_recv()
        arrived(0)

        @pl.loop(1, peers // 2)
        def _(pair):
            k = 2 * pair
            copy(outgoing, got, sends, recvs, k).wait_recv()
            copy(outgoing, got, sends, recvs, k + 1).wait_recv()
            arrived(k)

    deliver(proj, out_in, got_in, send_in, recv_in)
    w_pad[...] = jnp.zeros_like(w_pad)
    w_pad[0:classes, :] = w_outer[...]
    bias_col = jnp.broadcast_to(bias[...], (blk, hid)).T
    tile_copy.wait()
    found_copy.wait()
    aggregate(proj, out_in, got_in, send_in, recv_in, acc_in)
    score(acc_in, inv, bias_col, w_pad, scores, blk)
    deliver(scores, out_sc, got_sc, send_sc, recv_sc)
    aggregate(scores, out_sc, got_sc, send_sc, recv_sc, acc_sc)
    out[...] = inv * acc_sc[0:classes, :]

    @pl.loop(1, peers)
    def _(k):
        copy(out_in, got_in, send_in, recv_in, k).wait_send()
        copy(out_sc, got_sc, send_sc, recv_sc, k).wait_send()


def on_device(
    n_dom, n_sub,
    features, w_inner, bias_inner, w_outer, bias_outer, tiles, tile_col, degrees, send_rows
):
    peers = n_dom * n_sub
    verts, hid = features.shape[0], w_inner.shape[1]
    classes = w_outer.shape[1]
    padded = 16 * ((classes + 15) // 16)
    blk = tiles.shape[2]
    columns = verts // blk + peers
    lanes = 128 * ((columns + 127) // 128)
    small = (
        features.T, w_inner, bias_inner[None, :], w_outer.T, degrees[None, :], send_rows[0], tile_col
    )
    relay = n_sub == 4
    lists_out = 6 * n_dom if relay else peers
    vmem = pl.BlockSpec(memory_space=pltpu.VMEM)
    bf16, f32 = jnp.bfloat16, jnp.float32
    agg = pl.pallas_call(
        functools.partial(relay_kernel if relay else direct_kernel, n_dom, n_sub),
        out_shape=pltpu.VMEM((classes, verts), f32),
        in_specs=[pl.BlockSpec(memory_space=pl.ANY)] * 8,
        out_specs=vmem,
        scratch_shapes=[pltpu.VMEM(each.shape, each.dtype) for each in small]
        + [
            pltpu.SemaphoreType.DMA((len(small) + PARTS,)),
            pltpu.VMEM((tiles.shape[0], lanes), jnp.int32),
            pltpu.SMEM((tiles.shape[0], lanes), jnp.int32),
            pltpu.SemaphoreType.DMA,
            pltpu.VMEM((hid, verts), bf16),
            pltpu.VMEM((lists_out, hid, blk), bf16),
            pltpu.VMEM((peers, hid, blk), bf16),
            pltpu.VMEM((hid, verts), f32),
            pltpu.VMEM((padded, hid), bf16),
            pltpu.VMEM((padded, verts), bf16),
            pltpu.VMEM((peers, padded, blk), bf16),
            pltpu.VMEM((peers, padded, blk), bf16),
            pltpu.VMEM((padded, verts), f32),
            pltpu.VMEM(tiles.shape, bf16),
            pltpu.SemaphoreType.DMA,
            pltpu.SemaphoreType.DMA((2 if relay else peers,)),
            pltpu.SemaphoreType.DMA(((n_sub + 2) * n_dom // 2 if relay else peers,)),
            pltpu.SemaphoreType.DMA if relay else pltpu.SemaphoreType.DMA((peers,)),
            pltpu.SemaphoreType.DMA((n_sub if relay else peers,)),
        ]
        + (
            [
                pltpu.VMEM((2, hid, verts), bf16),
                pltpu.VMEM((2, peers, blk), jnp.int32),
                pltpu.SemaphoreType.DMA,
                pltpu.SemaphoreType.DMA((2, HALVES)),
                pltpu.SemaphoreType.DMA,
                pltpu.SemaphoreType.DMA((2,)),
                pltpu.VMEM((columns, blk, verts), bf16),
                pltpu.VMEM((n_sub, verts, n_dom * blk), bf16),
                pltpu.SemaphoreType.REGULAR,
            ]
            if relay
            else []
        ),
        compiler_params=pltpu.CompilerParams(
            collective_id=0, has_side_effects=True, vmem_limit_bytes=56 * 1024 * 1024
        ),
    )(*small, tiles)
    return agg.T + bias_outer


def solution(mesh):
    return jax.shard_map(
        functools.partial(on_device, mesh.shape["dom"], mesh.shape["sub"]),
        mesh=mesh,
        in_specs=(
            P(("dom", "sub"), None),
            P(),
            P(),
            P(),
            P(),
            P(("dom", "sub"), None, None, None),
            P(("dom", "sub"), None),
            P(("dom", "sub")),
            P(("dom", "sub"), None, None),
        ),
        out_specs=P(("dom", "sub"), None),
        check_vma=False,
    )
```

```python
import functools

import jax
import jax.numpy as jnp
from jax import lax
from jax.experimental import pallas as pl
from jax.experimental.pallas import tpu as pltpu
from jax.sharding import PartitionSpec as P

MESH = pl.DeviceIdType.MESH
NT = (((1,), (1,)), ((), ()))
PARTS = 2
HALVES = 2


class Place:
    def __init__(self, n_dom, n_sub):
        self.n_dom, self.n_sub = n_dom, n_sub
        self.dom, self.sub = lax.axis_index("dom"), lax.axis_index("sub")
        self.mine = self.dom * n_sub + self.sub

    def flip(self, a):
        total, bit = 0, 1
        while bit < self.n_dom:
            total = total + lax.rem(lax.div(self.dom, bit) + lax.div(a, bit), 2) * bit
            bit *= 2
        return total

    def target(self, k):
        n_sub = self.n_sub
        return self.flip(lax.div(k, n_sub)), lax.rem(self.sub + lax.rem(k, n_sub), n_sub)

    def source(self, k):
        n_sub = self.n_sub
        return self.flip(lax.div(k, n_sub)) * n_sub + lax.rem(self.sub + n_sub - lax.rem(k, n_sub), n_sub)


def hot_of(first, second, lists, verts):
    slots = jnp.concatenate([lists[pl.ds(first, 1), :], lists[pl.ds(second, 1), :]], axis=1)
    hot = lax.broadcasted_iota(jnp.int32, (verts, slots.shape[1]), 0) == slots
    return jnp.where(hot, 1.0, 0.0).astype(jnp.bfloat16)


def taken(table, hot):
    return jnp.dot(table[...], hot, preferred_element_type=jnp.float32).astype(table.dtype)


def picked(first, second, table, lists):
    return taken(table, hot_of(first, second, lists, table.shape[-1]))


def add(acc, block, c0, c1, fresh, tiles, where_tile):
    rows, _, blk, _ = tiles.shape

    def tile(r, c):
        t = where_tile[r, c]
        found = tiles[r, jnp.maximum(t, 0)]
        return jnp.where(t >= 0, found, jnp.zeros_like(found))

    for r in range(0, rows, 2):
        weights = jnp.concatenate(
            [jnp.concatenate([tile(r + q, c0), tile(r + q, c1)], axis=1) for q in range(2)], axis=0
        )
        term = lax.dot_general(block, weights, NT, preferred_element_type=jnp.float32)
        span = slice(r * blk, (r + 2) * blk)
        acc[:, span] = term if fresh else acc[:, span] + term


def prologue(place, hbm, staged, tiles_hbm, tiles, tile_sem, stage_sem, found, where_tile, found_sem, proj, greet):
    ft, w_inner, _, _, degrees, _, tile_col = staged
    verts = proj.shape[1]
    part = verts // PARTS
    small = [
        pltpu.make_async_copy(src, dst, stage_sem.at[i])
        for i, (src, dst) in enumerate(zip(hbm, staged))
        if i
    ]
    wide = [
        pltpu.make_async_copy(
            hbm[0].at[:, pl.ds(v * part, part)], ft.at[:, pl.ds(v * part, part)], stage_sem.at[len(staged) + v]
        )
        for v in range(PARTS)
    ]
    small[0].start()
    small[3].start()
    for each in wide:
        each.start()
    for i in (1, 2, 4, 5):
        small[i].start()
    tile_copy = pltpu.make_async_copy(tiles_hbm, tiles, tile_sem)

    greet()

    small[0].wait()
    small[3].wait()
    inv = lax.rsqrt(degrees[...].astype(jnp.float32))
    w_t = w_inner[...].T
    for v in range(PARTS):
        span = slice(v * part, (v + 1) * part)
        wide[v].wait()
        term = jnp.dot(w_t, ft[:, span], preferred_element_type=jnp.float32)
        if v == PARTS - 1:
            tile_copy.start()
        proj[:, span] = (term * inv[:, span]).astype(proj.dtype)
    for i in (1, 2, 4, 5):
        small[i].wait()
    cols = tile_col[...]
    lane = lax.broadcasted_iota(jnp.int32, found.shape, 1)
    at = jnp.full(found.shape, -1, jnp.int32)
    for t in range(cols.shape[1]):
        at = jnp.where(cols[:, t:t + 1] == lane, t, at)
    found[...] = at
    found_copy = pltpu.make_async_copy(found, where_tile, found_sem)
    found_copy.start()
    return inv, tile_copy, found_copy


def turn_of(i, count):
    return count - 1 - lax.div(i, 2) - count // 2 * lax.rem(i, 2)


def partner_of(i, count):
    a = turn_of(i, count)
    return a + 1 - 2 * lax.rem(a, 2)


def score(acc_in, inv, bias_col, w_pad, scores, blk):
    for v in range(0, scores.shape[1], blk):
        span = slice(v, v + blk)
        scale = inv[:, span]
        hidden = scale * jnp.maximum(scale * acc_in[:, span] + bias_col, 0.0)
        scores[:, span] = jnp.dot(
            w_pad[...], hidden.astype(jnp.bfloat16), preferred_element_type=jnp.float32
        ).astype(scores.dtype)


def relay_kernel(n_dom, n_sub, *refs):
    hbm, (tiles_hbm, out), staged, refs = refs[:7], refs[7:9], refs[9:16], refs[16:]
    (
        stage_sem, found, where_tile, found_sem, proj, out_in, got_in, acc_in, w_pad, scores, out_sc, got_sc,
        acc_sc, tiles, tile_sem, send_in, recv_in, send_sc, recv_sc, far_proj, far_lists, proj_send, proj_recv,
        lists_send, lists_recv, dense, hots, clear,
        passed_hots, far_scores, table_send, table_recv,
    ) = refs
    _, _, bias, w_outer, _, lists, _ = staged
    place = Place(n_dom, n_sub)
    dom, sub, flip = place.dom, place.sub, place.flip
    hid, verts = proj.shape
    blk = tiles.shape[2]
    own = verts // blk
    classes = w_outer.shape[0]
    part = hid // HALVES
    pairs = n_dom // 2
    per_step = 2 * n_dom
    peers = n_dom * n_sub
    half = lax.div(sub, 2)
    sibling, near, far = 1 + 4 * half - sub, 2 - half, 3 - 3 * half
    mid = lax.rem(sub + half, 2)
    middle, edge = mid == 1, mid == 0
    barrier = pltpu.get_barrier_semaphore()

    def greet():
        doms = [lax.rem(dom + d, n_dom) for d in range(n_dom)]
        for step in range(1, n_sub + 1):
            to_sub = lax.rem(sub + step, n_sub)
            for to_dom in doms[step // n_sub:]:
                pl.semaphore_signal(barrier, inc=1, device_id=(to_dom, to_sub), device_id_type=MESH)

    inv, tile_copy, found_copy = prologue(
        place, hbm, staged, tiles_hbm, tiles, tile_sem, stage_sem, found, where_tile, found_sem, proj, greet
    )

    def lists_copy(slot):
        return pltpu.make_async_remote_copy(
            src_ref=lists, dst_ref=far_lists.at[slot], send_sem=lists_send, recv_sem=lists_recv.at[slot],
            device_id=(dom, near), device_id_type=MESH,
        )

    def piece_copy(slot, c):
        rows = pl.ds(c * part, part)
        return pltpu.make_async_remote_copy(
            src_ref=proj.at[rows], dst_ref=far_proj.at[slot, rows], send_sem=proj_send,
            recv_sem=proj_recv.at[slot, c], device_id=(dom, near), device_id_type=MESH,
        )

    def send_table(slot):
        lists_copy(slot).start()
        for c in range(HALVES):
            piece_copy(slot, c).start()

    def await_table():
        lists_copy(0).wait_send()
        pltpu.make_async_remote_copy(
            src_ref=proj, dst_ref=far_proj.at[0], send_sem=proj_send, recv_sem=proj_recv.at[0, 0],
            device_id=(dom, near), device_id_type=MESH,
        ).wait_send()

    def came_in(plane, m, c):
        return recv_in.at[(n_sub * pairs + lax.rem(plane, 2) * pairs if c else plane * pairs) + m]

    def lists_of(ref, at, c):
        return ref.at[at] if c is None else ref.at[at, pl.ds(c * part, part)]

    def list_copy(j, plane, a, c, to_sub, relayed):
        return pltpu.make_async_remote_copy(
            src_ref=lists_of(out_in, j, c), dst_ref=lists_of(got_in, plane * n_dom + a, c),
            send_sem=send_in.at[relayed], recv_sem=came_in(plane, lax.div(a, 2), c),
            device_id=(flip(a), to_sub), device_id_type=MESH,
        )

    def await_lists(plane, m, c, count=2):
        at = pl.ds(plane * n_dom + 2 * m + 2 - count, count)
        pltpu.make_async_remote_copy(
            src_ref=lists_of(out_in, pl.ds(0, count), c), dst_ref=lists_of(got_in, at, c),
            send_sem=send_in.at[0], recv_sem=came_in(plane, m, c),
            device_id=(dom, sibling), device_id_type=MESH,
        ).wait_recv()

    def await_sent(relayed, count):
        pltpu.make_async_remote_copy(
            src_ref=out_in.at[pl.ds(0, count)], dst_ref=out_in.at[pl.ds(0, count)],
            send_sem=send_in.at[relayed], recv_sem=recv_in.at[0],
            device_id=(dom, sibling), device_id_type=MESH,
        ).wait_send()

    def keep_hot(a, hot, first, second):
        at = pl.ds(pl.multiple_of(a * blk, blk), blk)
        hots[first, :, at] = hot[:, :blk]
        hots[second, :, at] = hot[:, blk:]

    def pick_own(a):
        row = flip(a) * n_sub
        hot = hot_of(row + sub, row + sibling, lists, verts)
        keep_hot(a, hot, sub, sibling)
        both = taken(proj, hot)
        out_in[2 * a + 1] = both[:, blk:]
        return both[:, :blk]

    def pick_both(a):
        mine = pick_own(a)
        out_in[2 * a] = mine

        @pl.when(a == 0)
        def _():
            got_in[sub * n_dom] = mine

    def send_both(a):
        list_copy(2 * a + 1, sub, a, None, sibling, 0).start()
        pl.when(a != 0)(lambda: list_copy(2 * a, sub, a, None, sub, 0).start())

    def hand_out_own():
        send_both(partner_of(0, n_dom))

        @pl.loop(1, n_dom)
        def _(i):
            a = partner_of(i, n_dom)
            pick_both(a)
            send_both(a)

    def turn(begin, end, column_of, at):
        def tile(r, c):
            t = where_tile[r, c]
            found = tiles[r, jnp.maximum(t, 0)]
            return jnp.where(t >= 0, found, jnp.zeros_like(found))

        @pl.loop(begin, end)
        def _(i):
            c = column_of(i)
            for r in range(0, tiles.shape[0], 2):
                both = jnp.concatenate([tile(r, c), tile(r + 1, c)], axis=0)
                dense[at + i, :, r * blk:(r + 2) * blk] = both.T

    def turn_slots(begin, end):
        turn(begin, end, lambda i: own + flip(lax.rem(i, n_dom)) * n_sub + lax.div(i, n_dom), own)

    def keep_far_hots():
        @pl.loop(0, n_dom)
        def _(a):
            row = flip(a) * n_sub
            keep_hot(a, hot_of(row + near, row + far, lists, verts), near, far)

    def relay(slot, c, plane):
        if c == 0:
            lists_copy(slot).wait_recv()
        piece_copy(slot, c).wait_recv()
        base = (slot + 1) * per_step
        rows = slice(c * part, (c + 1) * part)

        def pair(a):
            row = flip(a) * n_sub
            at = pl.ds(pl.multiple_of(a * blk, blk), blk)
            if c == 0 or slot == 0:
                hot = hot_of(row + sub, row + sibling, far_lists.at[slot], verts)
                if slot == 1:
                    passed_hots[0, :, at] = hot[:, :blk]
                    passed_hots[1, :, at] = hot[:, blk:]
            else:
                hot = jnp.concatenate([passed_hots[0, :, at], passed_hots[1, :, at]], axis=1)
            return taken(far_proj.at[slot, rows], hot)

        @pl.loop(0, n_dom)
        def _(i):
            a = partner_of(i, n_dom)
            both = pair(a)
            j = base + 2 * a
            out_in[j, rows, :] = both[:, :blk]
            out_in[j + 1, rows, :] = both[:, blk:]
            list_copy(j + 1, plane, a, c, sibling, 1).start()
            pl.when(a != 0)(lambda: list_copy(j, plane, a, c, sub, 1).start())

            @pl.when(a == 0)
            def _():
                got_in[plane * n_dom, rows, :] = both[:, :blk]

    wide = 2 * blk

    def add_dense(acc, block, first, count, fresh):
        for v in range(0, verts, wide):
            span = slice(v, v + wide)
            weights = dense[pl.ds(first, count), :, span].reshape(count * blk, wide)
            term = jnp.dot(block, weights, preferred_element_type=jnp.float32)
            acc[:, span] = term if fresh else acc[:, span] + term

    def add_own(table, acc):
        add_dense(acc, table[...], 0, own, True)

    def add_pair(plane, m):
        slot = plane * n_dom + 2 * m
        add_dense(acc_in, jnp.concatenate([got_in[slot], got_in[slot + 1]], axis=1), own + slot, 2, False)

    def add_plane(plane, halves, local):
        parts = range(HALVES) if halves else (None,)

        @pl.loop(0, pairs - 1)
        def _(i):
            m = turn_of(i, pairs)
            for c in parts:
                await_lists(plane, m, c)
            add_pair(plane, m)

        for c in parts:
            await_lists(plane, 0, c, 1 if local else 2)
        add_pair(plane, 0)

    def add_halves(plane, c):
        rows = slice(c * part, (c + 1) * part)

        @pl.loop(0, pairs)
        def _(i):
            m = turn_of(i, pairs)
            slot = plane * n_dom + 2 * m
            await_lists(plane, m, c)
            block = jnp.concatenate([got_in[slot, rows, :], got_in[slot + 1, rows, :]], axis=1)
            add_dense(acc_in.at[rows], block, own + slot, 2, False)

    pick_both(partner_of(0, n_dom))
    pl.semaphore_wait(barrier, peers - 1)
    pl.when(middle)(lambda: send_table(0))
    hand_out_own()
    w_pad[...] = jnp.zeros_like(w_pad)
    w_pad[0:classes, :] = w_outer[...]
    bias_col = jnp.broadcast_to(bias[...], (blk, hid)).T
    tile_copy.wait()
    found_copy.wait()
    turn(0, own, lambda i: i, 0)
    turn_slots(0, n_dom)
    keep_far_hots()

    @pl.when(middle)
    def _():
        relay(0, 0, near)
        turn_slots(n_dom, 2 * n_dom)
        await_table()
        pl.semaphore_signal(clear, inc=1, device_id=(dom, sibling), device_id_type=MESH)
        turn_slots(2 * n_dom, peers)
        relay(0, 1, near)
        add_own(proj, acc_in)
        add_plane(sub, False, True)
        relay(1, 0, far)
        add_plane(sibling, False, False)
        relay(1, 1, far)
        add_plane(near, True, True)
        add_plane(far, True, True)

    @pl.when(edge)
    def _():
        turn_slots(n_dom, peers)
        add_own(proj, acc_in)
        pl.semaphore_wait(clear, 1)
        send_table(1)
        add_plane(sub, False, True)
        add_plane(sibling, False, False)
        add_halves(near, 0)
        add_halves(near, 1)
        add_halves(far, 0)
        add_halves(far, 1)

    score(acc_in, inv, bias_col, w_pad, scores, blk)

    order = [n_dom - 1 - i // 2 - n_dom // 2 * (i % 2) for i in range(n_dom)]
    order = [a + 1 - 2 * (a % 2) for a in order]

    def score_copy(k, source, a, plane):
        return pltpu.make_async_remote_copy(
            src_ref=out_sc.at[k], dst_ref=got_sc.at[source * n_dom + a], send_sem=send_sc,
            recv_sem=recv_sc.at[source], device_id=(flip(a), plane), device_id_type=MESH,
        )

    def give(table, hot, base, source, plane, local):
        lists_for = taken(table, hot)
        for a in order:
            one = lists_for[:, a * blk:(a + 1) * blk]
            out_sc[base + a] = one
            if a or local is False:
                score_copy(base + a, source, a, plane).start()
            elif local is True:
                got_sc[source * n_dom] = one
            else:
                pl.when(jnp.logical_not(local))(lambda: score_copy(base, source, 0, plane).start())

                @pl.when(local)
                def _():
                    got_sc[source * n_dom] = one

    def deliver(plane):
        give(scores, hots[plane], plane * n_dom, sub, plane, sub == plane)

    def table_copy():
        return pltpu.make_async_remote_copy(
            src_ref=scores, dst_ref=far_scores, send_sem=table_send, recv_sem=table_recv,
            device_id=(dom, near), device_id_type=MESH,
        )

    def pass_scores():
        table_copy().wait_recv()
        give(far_scores, passed_hots[1], peers, 0, sibling, False)
        give(far_scores, passed_hots[0], peers + n_dom, 0, sub, True)

    def scores_wait(at, count, plane):
        return pltpu.make_async_remote_copy(
            src_ref=out_sc.at[pl.ds(0, count)], dst_ref=got_sc.at[pl.ds(at, count)], send_sem=send_sc,
            recv_sem=recv_sc.at[plane], device_id=(dom, sibling), device_id_type=MESH,
        )

    def scores_sent(count):
        pltpu.make_async_remote_copy(
            src_ref=out_sc.at[pl.ds(0, count)], dst_ref=out_sc.at[pl.ds(0, count)], send_sem=send_sc,
            recv_sem=recv_sc.at[0], device_id=(dom, sibling), device_id_type=MESH,
        ).wait_send()

    def gather(plane):
        slot = plane * n_dom
        local = jnp.logical_or(plane == sub, jnp.logical_and(plane == 0, sub == 2))
        pl.when(jnp.logical_not(local))(lambda: scores_wait(slot, n_dom, plane).wait_recv())
        pl.when(local)(lambda: scores_wait(slot + 1, n_dom - 1, plane).wait_recv())
        block = jnp.concatenate([got_sc[slot + a] for a in range(n_dom)], axis=1)
        add_dense(acc_sc, block, own + slot, n_dom, False)

    @pl.when(middle)
    def _():
        for plane in (near, far, sibling, sub):
            deliver(plane)

    @pl.when(sub == 0)
    def _():
        table_copy().start()
        for plane in (sub, sibling):
            deliver(plane)

    @pl.when(sub == 3)
    def _():
        for plane in (far, sub, near, sibling):
            deliver(plane)

    add_own(scores, acc_sc)
    await_sent(0, per_step - 1)
    pl.when(edge)(await_table)
    pl.when(middle)(lambda: await_sent(1, 2 * (per_step - 1)))
    gather(sibling + mid * (sub - sibling))
    gather(near)
    pl.when(sub == 2)(pass_scores)
    last = lax.div(sub, 3)
    gather(3 * last)
    gather(3 - 3 * last)
    out[...] = inv * acc_sc[0:classes, :]

    @pl.when(sub == 0)
    def _():
        table_copy().wait_send()
        scores_sent(2 * n_dom - 1)

    pl.when(lax.rem(sub, 2) == 1)(lambda: scores_sent(peers - 1))
    pl.when(sub == 2)(lambda: scores_sent(peers + 2 * n_dom - 2))


def direct_kernel(n_dom, n_sub, *refs):
    hbm, (tiles_hbm, out), staged, refs = refs[:7], refs[7:9], refs[9:16], refs[16:]
    (
        stage_sem, found, where_tile, found_sem, proj, out_in, got_in, acc_in, w_pad, scores, out_sc, got_sc,
        acc_sc, tiles, tile_sem, send_in, recv_in, send_sc, recv_sc,
    ) = refs
    _, _, bias, w_outer, _, lists, _ = staged
    place = Place(n_dom, n_sub)
    peers = n_dom * n_sub
    hid, verts = proj.shape
    blk = tiles.shape[2]
    own = verts // blk
    classes = w_outer.shape[0]

    barrier = pltpu.get_barrier_semaphore()

    def greet():
        @pl.loop(1, peers)
        def _(k):
            pl.semaphore_signal(barrier, inc=1, device_id=place.target(k), device_id_type=MESH)

    inv, tile_copy, found_copy = prologue(
        place, hbm, staged, tiles_hbm, tiles, tile_sem, stage_sem, found, where_tile, found_sem, proj, greet
    )
    pl.semaphore_wait(barrier, peers - 1)

    def copy(src, dst, sends, recvs, k):
        return pltpu.make_async_remote_copy(
            src_ref=src.at[k], dst_ref=dst.at[k], send_sem=sends.at[k], recv_sem=recvs.at[k],
            device_id=place.target(k), device_id_type=MESH,
        )

    def pick(k, table):
        index = [to_dom * n_sub + to_sub for to_dom, to_sub in (place.target(k), place.target(k + 1))]
        return picked(*index, table, lists)

    def deliver(table, outgoing, got, sends, recvs):
        first = pick(0, table)
        got[0] = first[:, :blk]
        outgoing[1] = first[:, blk:]
        copy(outgoing, got, sends, recvs, 1).start()

        @pl.loop(1, peers // 2)
        def _(pair):
            k = 2 * pair
            both = pick(k, table)
            outgoing[k] = both[:, :blk]
            outgoing[k + 1] = both[:, blk:]
            copy(outgoing, got, sends, recvs, k).start()
            copy(outgoing, got, sends, recvs, k + 1).start()

    def aggregate(table, outgoing, got, sends, recvs, acc):
        for c in range(0, own, 2):
            add(acc, table[:, c * blk:(c + 2) * blk], c, c + 1, c == 0, tiles, where_tile)

        def arrived(k):
            block = jnp.concatenate([got[k], got[k + 1]], axis=1)
            add(acc, block, own + place.source(k), own + place.source(k + 1), False, tiles, where_tile)

        copy(outgoing, got, sends, recvs, 1).wait_recv()
        arrived(0)

        @pl.loop(1, peers // 2)
        def _(pair):
            k = 2 * pair
            copy(outgoing, got, sends, recvs, k).wait_recv()
            copy(outgoing, got, sends, recvs, k + 1).wait_recv()
            arrived(k)

    deliver(proj, out_in, got_in, send_in, recv_in)
    w_pad[...] = jnp.zeros_like(w_pad)
    w_pad[0:classes, :] = w_outer[...]
    bias_col = jnp.broadcast_to(bias[...], (blk, hid)).T
    tile_copy.wait()
    found_copy.wait()
    aggregate(proj, out_in, got_in, send_in, recv_in, acc_in)
    score(acc_in, inv, bias_col, w_pad, scores, blk)
    deliver(scores, out_sc, got_sc, send_sc, recv_sc)
    aggregate(scores, out_sc, got_sc, send_sc, recv_sc, acc_sc)
    out[...] = inv * acc_sc[0:classes, :]

    @pl.loop(1, peers)
    def _(k):
        copy(out_in, got_in, send_in, recv_in, k).wait_send()
        copy(out_sc, got_sc, send_sc, recv_sc, k).wait_send()


def on_device(
    n_dom, n_sub,
    features, w_inner, bias_inner, w_outer, bias_outer, tiles, tile_col, degrees, send_rows
):
    peers = n_dom * n_sub
    verts, hid = features.shape[0], w_inner.shape[1]
    classes = w_outer.shape[1]
    padded = 16 * ((classes + 15) // 16)
    blk = tiles.shape[2]
    columns = verts // blk + peers
    lanes = 128 * ((columns + 127) // 128)
    small = (
        features.T, w_inner, bias_inner[None, :], w_outer.T, degrees[None, :], send_rows[0], tile_col
    )
    relay = n_sub == 4
    lists_out = 6 * n_dom if relay else peers
    vmem = pl.BlockSpec(memory_space=pltpu.VMEM)
    bf16, f32 = jnp.bfloat16, jnp.float32
    agg = pl.pallas_call(
        functools.partial(relay_kernel if relay else direct_kernel, n_dom, n_sub),
        out_shape=pltpu.VMEM((classes, verts), f32),
        in_specs=[pl.BlockSpec(memory_space=pl.ANY)] * 8,
        out_specs=vmem,
        scratch_shapes=[pltpu.VMEM(each.shape, each.dtype) for each in small]
        + [
            pltpu.SemaphoreType.DMA((len(small) + PARTS,)),
            pltpu.VMEM((tiles.shape[0], lanes), jnp.int32),
            pltpu.SMEM((tiles.shape[0], lanes), jnp.int32),
            pltpu.SemaphoreType.DMA,
            pltpu.VMEM((hid, verts), bf16),
            pltpu.VMEM((lists_out, hid, blk), bf16),
            pltpu.VMEM((peers, hid, blk), bf16),
            pltpu.VMEM((hid, verts), f32),
            pltpu.VMEM((padded, hid), bf16),
            pltpu.VMEM((padded, verts), bf16),
            pltpu.VMEM((peers + 2 * n_dom if relay else peers, padded, blk), bf16),
            pltpu.VMEM((peers, padded, blk), bf16),
            pltpu.VMEM((padded, verts), f32),
            pltpu.VMEM(tiles.shape, bf16),
            pltpu.SemaphoreType.DMA,
            pltpu.SemaphoreType.DMA((2 if relay else peers,)),
            pltpu.SemaphoreType.DMA(((n_sub + 2) * n_dom // 2 if relay else peers,)),
            pltpu.SemaphoreType.DMA if relay else pltpu.SemaphoreType.DMA((peers,)),
            pltpu.SemaphoreType.DMA((n_sub if relay else peers,)),
        ]
        + (
            [
                pltpu.VMEM((2, hid, verts), bf16),
                pltpu.VMEM((2, peers, blk), jnp.int32),
                pltpu.SemaphoreType.DMA,
                pltpu.SemaphoreType.DMA((2, HALVES)),
                pltpu.SemaphoreType.DMA,
                pltpu.SemaphoreType.DMA((2,)),
                pltpu.VMEM((columns, blk, verts), bf16),
                pltpu.VMEM((n_sub, verts, n_dom * blk), bf16),
                pltpu.SemaphoreType.REGULAR,
                pltpu.VMEM((2, verts, n_dom * blk), bf16),
                pltpu.VMEM((padded, verts), bf16),
                pltpu.SemaphoreType.DMA,
                pltpu.SemaphoreType.DMA,
            ]
            if relay
            else []
        ),
        compiler_params=pltpu.CompilerParams(
            collective_id=0, has_side_effects=True, vmem_limit_bytes=56 * 1024 * 1024
        ),
    )(*small, tiles)
    return agg.T + bias_outer


def solution(mesh):
    return jax.shard_map(
        functools.partial(on_device, mesh.shape["dom"], mesh.shape["sub"]),
        mesh=mesh,
        in_specs=(
            P(("dom", "sub"), None),
            P(),
            P(),
            P(),
            P(),
            P(("dom", "sub"), None, None, None),
            P(("dom", "sub"), None),
            P(("dom", "sub")),
            P(("dom", "sub"), None, None),
        ),
        out_specs=P(("dom", "sub"), None),
        check_vma=False,
    )
```

```python
import functools

import jax
import jax.numpy as jnp
from jax import lax
from jax.experimental import pallas as pl
from jax.experimental.pallas import tpu as pltpu
from jax.sharding import PartitionSpec as P

MESH = pl.DeviceIdType.MESH
NT = (((1,), (1,)), ((), ()))
PARTS = 2
HALVES = 2


class Place:
    def __init__(self, n_dom, n_sub):
        self.n_dom, self.n_sub = n_dom, n_sub
        self.dom, self.sub = lax.axis_index("dom"), lax.axis_index("sub")
        self.mine = self.dom * n_sub + self.sub

    def flip(self, a):
        total, bit = 0, 1
        while bit < self.n_dom:
            total = total + lax.rem(lax.div(self.dom, bit) + lax.div(a, bit), 2) * bit
            bit *= 2
        return total

    def target(self, k):
        n_sub = self.n_sub
        return self.flip(lax.div(k, n_sub)), lax.rem(self.sub + lax.rem(k, n_sub), n_sub)

    def source(self, k):
        n_sub = self.n_sub
        return self.flip(lax.div(k, n_sub)) * n_sub + lax.rem(self.sub + n_sub - lax.rem(k, n_sub), n_sub)


def hot_of(first, second, lists, verts):
    slots = jnp.concatenate([lists[pl.ds(first, 1), :], lists[pl.ds(second, 1), :]], axis=1)
    hot = lax.broadcasted_iota(jnp.int32, (verts, slots.shape[1]), 0) == slots
    return jnp.where(hot, 1.0, 0.0).astype(jnp.bfloat16)


def taken(table, hot):
    return jnp.dot(table[...], hot, preferred_element_type=jnp.float32).astype(table.dtype)


def picked(first, second, table, lists):
    return taken(table, hot_of(first, second, lists, table.shape[-1]))


def add(acc, block, c0, c1, fresh, tiles, where_tile):
    rows, _, blk, _ = tiles.shape

    def tile(r, c):
        t = where_tile[r, c]
        found = tiles[r, jnp.maximum(t, 0)]
        return jnp.where(t >= 0, found, jnp.zeros_like(found))

    for r in range(0, rows, 2):
        weights = jnp.concatenate(
            [jnp.concatenate([tile(r + q, c0), tile(r + q, c1)], axis=1) for q in range(2)], axis=0
        )
        term = lax.dot_general(block, weights, NT, preferred_element_type=jnp.float32)
        span = slice(r * blk, (r + 2) * blk)
        acc[:, span] = term if fresh else acc[:, span] + term


def prologue(place, hbm, staged, tiles_hbm, tiles, tile_sem, stage_sem, proj, greet):
    ft, w_inner, _, _, degrees, _, _ = staged
    verts = proj.shape[1]
    part = verts // PARTS
    whole = ft.shape[0] // 256 * 256
    small = [
        pltpu.make_async_copy(src, dst, stage_sem.at[i])
        for i, (src, dst) in enumerate(zip(hbm, staged))
        if i
    ]
    wide = [
        pltpu.make_async_copy(
            hbm[0].at[:, pl.ds(v * part, part)], ft.at[:, pl.ds(v * part, part)], stage_sem.at[len(staged) + v]
        )
        for v in range(PARTS)
    ]
    small[0].start()
    small[3].start()
    for each in wide:
        each.start()
    for i in (1, 2, 4, 5):
        small[i].start()
    tile_copy = pltpu.make_async_copy(tiles_hbm, tiles, tile_sem)

    greet()

    small[0].wait()
    small[3].wait()
    inv = lax.rsqrt(degrees[...].astype(jnp.float32))
    w_t = w_inner[...].T
    for v in range(PARTS):
        span = slice(v * part, (v + 1) * part)
        wide[v].wait()
        term = jnp.dot(w_t[:, :whole], ft[:whole, span], preferred_element_type=jnp.float32)
        if whole < ft.shape[0]:
            term += jnp.dot(w_t[:, whole:], ft[whole:, span], preferred_element_type=jnp.float32)
        if v == PARTS - 1:
            tile_copy.start()
        proj[:, span] = (term * inv[:, span]).astype(proj.dtype)
    for i in (1, 2, 4, 5):
        small[i].wait()
    return inv, tile_copy


def place_tiles(tile_col, found, where_tile, found_sem):
    cols = tile_col[...]
    lane = lax.broadcasted_iota(jnp.int32, found.shape, 1)
    at = jnp.full(found.shape, -1, jnp.int32)
    for t in range(cols.shape[1]):
        at = jnp.where(cols[:, t:t + 1] == lane, t, at)
    found[...] = at
    found_copy = pltpu.make_async_copy(found, where_tile, found_sem)
    found_copy.start()
    return found_copy


def turn_of(i, count):
    return count - 1 - lax.div(i, 2) - count // 2 * lax.rem(i, 2)


def partner_of(i, count):
    a = turn_of(i, count)
    return a + 1 - 2 * lax.rem(a, 2)


def score(acc_in, inv, bias_col, w_pad, scores, blk):
    for v in range(0, scores.shape[1], blk):
        span = slice(v, v + blk)
        scale = inv[:, span]
        hidden = scale * jnp.maximum(scale * acc_in[:, span] + bias_col, 0.0)
        scores[:, span] = jnp.dot(
            w_pad[...], hidden.astype(jnp.bfloat16), preferred_element_type=jnp.float32
        ).astype(scores.dtype)


def relay_kernel(n_dom, n_sub, *refs):
    hbm, (tiles_hbm, out), staged, refs = refs[:7], refs[7:9], refs[9:16], refs[16:]
    (
        stage_sem, found, where_tile, found_sem, proj, out_in, got_in, acc_in, w_pad, scores, out_sc, got_sc,
        acc_sc, tiles, tile_sem, send_in, recv_in, send_sc, recv_sc, far_proj, far_lists, proj_send, proj_recv,
        lists_send, lists_recv, dense, hots, clear,
        passed_hots, far_scores, table_send, table_recv,
    ) = refs
    _, _, bias, w_outer, _, lists, _ = staged
    place = Place(n_dom, n_sub)
    dom, sub, flip = place.dom, place.sub, place.flip
    hid, verts = proj.shape
    blk = tiles.shape[2]
    own = verts // blk
    classes = w_outer.shape[0]
    part = hid // HALVES
    pairs = n_dom // 2
    per_step = 2 * n_dom
    peers = n_dom * n_sub
    half = lax.div(sub, 2)
    sibling, near, far = 1 + 4 * half - sub, 2 - half, 3 - 3 * half
    mid = lax.rem(sub + half, 2)
    middle, edge = mid == 1, mid == 0
    barrier = pltpu.get_barrier_semaphore()

    def greet():
        doms = [lax.rem(dom + d, n_dom) for d in range(n_dom)]
        for step in range(1, n_sub + 1):
            to_sub = lax.rem(sub + step, n_sub)
            for to_dom in doms[step // n_sub:]:
                pl.semaphore_signal(barrier, inc=1, device_id=(to_dom, to_sub), device_id_type=MESH)

    inv, tile_copy = prologue(place, hbm, staged, tiles_hbm, tiles, tile_sem, stage_sem, proj, greet)

    def lists_copy(slot):
        return pltpu.make_async_remote_copy(
            src_ref=lists, dst_ref=far_lists.at[slot], send_sem=lists_send, recv_sem=lists_recv.at[slot],
            device_id=(dom, near), device_id_type=MESH,
        )

    def piece_copy(slot, c):
        rows = pl.ds(c * part, part)
        return pltpu.make_async_remote_copy(
            src_ref=proj.at[rows], dst_ref=far_proj.at[slot, rows], send_sem=proj_send,
            recv_sem=proj_recv.at[slot, c], device_id=(dom, near), device_id_type=MESH,
        )

    def send_table(slot):
        lists_copy(slot).start()
        for c in range(HALVES):
            piece_copy(slot, c).start()

    def await_table():
        lists_copy(0).wait_send()
        pltpu.make_async_remote_copy(
            src_ref=proj, dst_ref=far_proj.at[0], send_sem=proj_send, recv_sem=proj_recv.at[0, 0],
            device_id=(dom, near), device_id_type=MESH,
        ).wait_send()

    def came_in(plane, m, c, slot):
        return recv_in.at[lax.rem(plane, 2) if c is None else 2 + HALVES * slot + c + (m if slot and c else 0)]

    def lists_of(ref, at, c):
        return ref.at[at] if c is None else ref.at[at, pl.ds(c * part, part)]

    def list_copy(j, plane, a, c, to_sub, slot=None):
        return pltpu.make_async_remote_copy(
            src_ref=lists_of(out_in, j, c), dst_ref=lists_of(got_in, plane * n_dom + a, c),
            send_sem=send_in.at[0 if slot is None else 1], recv_sem=came_in(plane, lax.div(a, 2), c, slot),
            device_id=(flip(a), to_sub), device_id_type=MESH,
        )

    def await_lists(plane, a, count, c, slot=None):
        pltpu.make_async_remote_copy(
            src_ref=lists_of(out_in, pl.ds(0, count), c),
            dst_ref=lists_of(got_in, pl.ds(plane * n_dom + a, count), c),
            send_sem=send_in.at[0], recv_sem=came_in(plane, lax.div(a, 2), c, slot),
            device_id=(dom, sibling), device_id_type=MESH,
        ).wait_recv()

    def await_sent(relayed, count):
        pltpu.make_async_remote_copy(
            src_ref=out_in.at[pl.ds(0, count)], dst_ref=out_in.at[pl.ds(0, count)],
            send_sem=send_in.at[relayed], recv_sem=recv_in.at[0],
            device_id=(dom, sibling), device_id_type=MESH,
        ).wait_send()

    def keep_hot(a, hot, first, second):
        at = pl.ds(pl.multiple_of(a * blk, blk), blk)
        hots[first, :, at] = hot[:, :blk]
        hots[second, :, at] = hot[:, blk:]

    def pick_own(a):
        row = flip(a) * n_sub
        hot = hot_of(row + sub, row + sibling, lists, verts)
        keep_hot(a, hot, sub, sibling)
        both = taken(proj, hot)
        out_in[2 * a + 1] = both[:, blk:]
        return both[:, :blk]

    def pick_both(a):
        mine = pick_own(a)
        out_in[2 * a] = mine

        @pl.when(a == 0)
        def _():
            got_in[sub * n_dom] = mine

    def send_both(a):
        list_copy(2 * a + 1, sub, a, None, sibling).start()
        pl.when(a != 0)(lambda: list_copy(2 * a, sub, a, None, sub).start())

    def hand_out_own():
        send_both(partner_of(0, n_dom))

        @pl.loop(1, n_dom)
        def _(i):
            a = partner_of(i, n_dom)
            pick_both(a)
            send_both(a)

    def turn(begin, end, column_of, at):
        def tile(r, c):
            t = where_tile[r, c]
            found = tiles[r, jnp.maximum(t, 0)]
            return jnp.where(t >= 0, found, jnp.zeros_like(found))

        @pl.loop(begin, end)
        def _(i):
            c = column_of(i)
            for r in range(0, tiles.shape[0], 2):
                both = jnp.concatenate([tile(r, c), tile(r + 1, c)], axis=0)
                dense[at + i, :, r * blk:(r + 2) * blk] = both.T

    def turn_slots(begin, end):
        turn(begin, end, lambda i: own + flip(lax.rem(i, n_dom)) * n_sub + lax.div(i, n_dom), own)

    def keep_far_hots():
        @pl.loop(0, n_dom)
        def _(a):
            row = flip(a) * n_sub
            keep_hot(a, hot_of(row + near, row + far, lists, verts), near, far)

    def relay(slot, c, plane):
        if c == 0:
            lists_copy(slot).wait_recv()
        piece_copy(slot, c).wait_recv()
        base = (slot + 1) * per_step
        rows = slice(c * part, (c + 1) * part)

        def pair(a):
            row = flip(a) * n_sub
            at = pl.ds(pl.multiple_of(a * blk, blk), blk)
            if c == 0:
                hot = hot_of(row + sub, row + sibling, far_lists.at[slot], verts)
                passed_hots[slot, 0, :, at] = hot[:, :blk]
                passed_hots[slot, 1, :, at] = hot[:, blk:]
            else:
                hot = jnp.concatenate([passed_hots[slot, 0, :, at], passed_hots[slot, 1, :, at]], axis=1)
            return taken(far_proj.at[slot, rows], hot)

        @pl.loop(0, n_dom)
        def _(i):
            a = partner_of(i, n_dom)
            both = pair(a)
            j = base + 2 * a
            out_in[j, rows, :] = both[:, :blk]
            out_in[j + 1, rows, :] = both[:, blk:]
            list_copy(j + 1, plane, a, c, sibling, slot).start()
            pl.when(a != 0)(lambda: list_copy(j, plane, a, c, sub, slot).start())

            @pl.when(a == 0)
            def _():
                got_in[plane * n_dom, rows, :] = both[:, :blk]

    def add_dense(acc, block, first, count, fresh):
        wide = 2 * blk if acc.shape[0] >= part else 8 * blk
        for v in range(0, verts, wide):
            span = slice(v, v + wide)
            weights = dense[pl.ds(first, count), :, span].reshape(count * blk, wide)
            term = jnp.dot(block, weights, preferred_element_type=jnp.float32)
            acc[:, span] = term if fresh else acc[:, span] + term

    def add_own(table, acc):
        add_dense(acc, table[...], 0, own, True)

    def add_pair(plane, m):
        slot = plane * n_dom + 2 * m
        add_dense(acc_in, jnp.concatenate([got_in[slot], got_in[slot + 1]], axis=1), own + slot, 2, False)

    def add_pairs(plane):
        @pl.loop(0, pairs)
        def _(i):
            add_pair(plane, turn_of(i, pairs))

    def add_plane(plane, local):
        await_lists(plane, local, n_dom - local, None)
        add_pairs(plane)

    def add_passed(slot, plane):
        await_lists(plane, 1, n_dom - 1, 0, slot)
        if slot:
            for m in range(pairs):
                await_lists(plane, 2 * m if m else 1, 2 if m else 1, 1, slot)
        else:
            await_lists(plane, 1, n_dom - 1, 1, slot)
        add_pairs(plane)

    def add_halves(slot, plane, c):
        rows = slice(c * part, (c + 1) * part)
        if not (slot and c):
            await_lists(plane, 0, n_dom, c, slot)

        @pl.loop(0, pairs)
        def _(i):
            m = turn_of(i, pairs)
            at = plane * n_dom + 2 * m
            if slot and c:
                await_lists(plane, 2 * m, 2, c, slot)
            block = jnp.concatenate([got_in[at, rows, :], got_in[at + 1, rows, :]], axis=1)
            add_dense(acc_in.at[rows], block, own + at, 2, False)

    pick_both(partner_of(0, n_dom))
    pl.semaphore_wait(barrier, peers - 1)
    pl.when(middle)(lambda: send_table(0))
    hand_out_own()
    found_copy = place_tiles(staged[6], found, where_tile, found_sem)
    w_pad[...] = jnp.zeros_like(w_pad)
    w_pad[0:classes, :] = w_outer[...]
    bias_col = jnp.broadcast_to(bias[...], (blk, hid)).T
    tile_copy.wait()
    found_copy.wait()
    turn(0, own, lambda i: i, 0)
    turn_slots(0, n_dom)
    keep_far_hots()

    @pl.when(middle)
    def _():
        relay(0, 0, near)
        turn_slots(n_dom, 2 * n_dom)
        await_table()
        pl.semaphore_signal(clear, inc=1, device_id=(dom, sibling), device_id_type=MESH)
        turn_slots(2 * n_dom, peers)
        relay(0, 1, near)
        add_own(proj, acc_in)
        add_plane(sub, 1)
        relay(1, 0, far)
        add_plane(sibling, 0)
        relay(1, 1, far)
        add_passed(0, near)
        add_passed(1, far)

    @pl.when(edge)
    def _():
        turn_slots(n_dom, peers)
        add_own(proj, acc_in)
        pl.semaphore_wait(clear, 1)
        send_table(1)
        add_plane(sub, 1)
        add_plane(sibling, 0)
        add_halves(0, near, 0)
        add_halves(0, near, 1)
        add_halves(1, far, 0)
        add_halves(1, far, 1)

    score(acc_in, inv, bias_col, w_pad, scores, blk)

    order = [n_dom - 1 - i // 2 - n_dom // 2 * (i % 2) for i in range(n_dom)]
    order = [a + 1 - 2 * (a % 2) for a in order]

    def score_copy(k, source, a, plane):
        return pltpu.make_async_remote_copy(
            src_ref=out_sc.at[k], dst_ref=got_sc.at[source * n_dom + a], send_sem=send_sc,
            recv_sem=recv_sc.at[source], device_id=(flip(a), plane), device_id_type=MESH,
        )

    def give(table, hot, base, source, plane, local):
        lists_for = taken(table, hot)
        for a in order:
            one = lists_for[:, a * blk:(a + 1) * blk]
            out_sc[base + a] = one
            if a or local is False:
                score_copy(base + a, source, a, plane).start()
            elif local is True:
                got_sc[source * n_dom] = one
            else:
                pl.when(jnp.logical_not(local))(lambda: score_copy(base, source, 0, plane).start())

                @pl.when(local)
                def _():
                    got_sc[source * n_dom] = one

    def deliver(plane):
        give(scores, hots[plane], plane * n_dom, sub, plane, sub == plane)

    def table_copy(slot):
        return pltpu.make_async_remote_copy(
            src_ref=scores, dst_ref=far_scores.at[slot], send_sem=table_send, recv_sem=table_recv.at[slot],
            device_id=(dom, near), device_id_type=MESH,
        )

    def pass_scores(slot, source, to_own, to_sibling):
        table_copy(slot).wait_recv()
        for own_plane in (slot == 1, slot == 0):
            if own_plane:
                give(far_scores.at[slot], passed_hots[slot, 0], to_own, source, sub, True)
            else:
                give(far_scores.at[slot], passed_hots[slot, 1], to_sibling, source, sibling, False)

    def scores_wait(at, count, plane):
        return pltpu.make_async_remote_copy(
            src_ref=out_sc.at[pl.ds(0, count)], dst_ref=got_sc.at[pl.ds(at, count)], send_sem=send_sc,
            recv_sem=recv_sc.at[plane], device_id=(dom, sibling), device_id_type=MESH,
        )

    def scores_sent(count):
        pltpu.make_async_remote_copy(
            src_ref=out_sc.at[pl.ds(0, count)], dst_ref=out_sc.at[pl.ds(0, count)], send_sem=send_sc,
            recv_sem=recv_sc.at[0], device_id=(dom, sibling), device_id_type=MESH,
        ).wait_send()

    def gather(plane):
        slot = plane * n_dom
        passed = jnp.logical_or(plane == near, jnp.logical_and(plane == 0, sub == 2))
        local = jnp.logical_or(plane == sub, jnp.logical_and(middle, passed))
        pl.when(jnp.logical_not(local))(lambda: scores_wait(slot, n_dom, plane).wait_recv())
        pl.when(local)(lambda: scores_wait(slot + 1, n_dom - 1, plane).wait_recv())
        block = jnp.concatenate([got_sc[slot + a] for a in range(n_dom)], axis=1)
        add_dense(acc_sc, block, own + slot, n_dom, False)

    @pl.when(middle)
    def _():
        table_copy(0).start()
        for plane in (sibling, sub):
            deliver(plane)

    @pl.when(sub == 0)
    def _():
        table_copy(1).start()
        deliver(sub)

    @pl.when(sub == 3)
    def _():
        for plane in (far, sub, near, sibling):
            deliver(plane)

    add_own(scores, acc_sc)
    await_sent(0, per_step - 1)
    pl.when(edge)(await_table)
    pl.when(middle)(lambda: pass_scores(0, near, near * n_dom, far * n_dom))
    pl.when(middle)(lambda: await_sent(1, 2 * (per_step - 1)))
    pl.when(sub == 0)(lambda: deliver(sibling))
    on = [lax.div(3 - sub, 3), 0, 0, lax.div(sub, 3)]
    on[1] = lax.rem(sub, 2) - on[3]
    on[2] = 1 - on[0] - on[1] - on[3]
    first, second, third, fourth = (
        sum(here * plane for here, plane in zip(on, planes))
        for planes in ((0, 1, 2, 2), (3, 2, 1, 1), (1, 0, 3, 3), (2, 3, 0, 0))
    )
    gather(first)
    pl.when(sub == 2)(lambda: pass_scores(1, 0, peers, peers + n_dom))
    gather(second)
    gather(third)
    gather(fourth)
    out[...] = inv * acc_sc[0:classes, :]

    @pl.when(sub == 0)
    def _():
        scores_sent(2 * n_dom - 1)

    pl.when(sub == 1)(lambda: scores_sent(peers - 2))
    pl.when(sub == 2)(lambda: scores_sent(peers + 2 * n_dom - 3))
    pl.when(sub == 3)(lambda: scores_sent(peers - 1))
    pl.when(sub != 3)(lambda: table_copy(0).wait_send())


def direct_kernel(n_dom, n_sub, *refs):
    hbm, (tiles_hbm, out), staged, refs = refs[:7], refs[7:9], refs[9:16], refs[16:]
    (
        stage_sem, found, where_tile, found_sem, proj, out_in, got_in, acc_in, w_pad, scores, out_sc, got_sc,
        acc_sc, tiles, tile_sem, send_in, recv_in, send_sc, recv_sc,
    ) = refs
    _, _, bias, w_outer, _, lists, _ = staged
    place = Place(n_dom, n_sub)
    peers = n_dom * n_sub
    hid, verts = proj.shape
    blk = tiles.shape[2]
    own = verts // blk
    classes = w_outer.shape[0]

    barrier = pltpu.get_barrier_semaphore()

    def greet():
        @pl.loop(1, peers)
        def _(k):
            pl.semaphore_signal(barrier, inc=1, device_id=place.target(k), device_id_type=MESH)

    inv, tile_copy = prologue(place, hbm, staged, tiles_hbm, tiles, tile_sem, stage_sem, proj, greet)
    pl.semaphore_wait(barrier, peers - 1)

    def copy(src, dst, sends, recvs, k):
        return pltpu.make_async_remote_copy(
            src_ref=src.at[k], dst_ref=dst.at[k], send_sem=sends.at[k], recv_sem=recvs.at[k],
            device_id=place.target(k), device_id_type=MESH,
        )

    def pick(k, table):
        index = [to_dom * n_sub + to_sub for to_dom, to_sub in (place.target(k), place.target(k + 1))]
        return picked(*index, table, lists)

    def deliver(table, outgoing, got, sends, recvs):
        first = pick(0, table)
        got[0] = first[:, :blk]
        outgoing[1] = first[:, blk:]
        copy(outgoing, got, sends, recvs, 1).start()

        @pl.loop(1, peers // 2)
        def _(pair):
            k = 2 * pair
            both = pick(k, table)
            outgoing[k] = both[:, :blk]
            outgoing[k + 1] = both[:, blk:]
            copy(outgoing, got, sends, recvs, k).start()
            copy(outgoing, got, sends, recvs, k + 1).start()

    def aggregate(table, outgoing, got, sends, recvs, acc):
        for c in range(0, own, 2):
            add(acc, table[:, c * blk:(c + 2) * blk], c, c + 1, c == 0, tiles, where_tile)

        def arrived(k):
            block = jnp.concatenate([got[k], got[k + 1]], axis=1)
            add(acc, block, own + place.source(k), own + place.source(k + 1), False, tiles, where_tile)

        copy(outgoing, got, sends, recvs, 1).wait_recv()
        arrived(0)

        @pl.loop(1, peers // 2)
        def _(pair):
            k = 2 * pair
            copy(outgoing, got, sends, recvs, k).wait_recv()
            copy(outgoing, got, sends, recvs, k + 1).wait_recv()
            arrived(k)

    deliver(proj, out_in, got_in, send_in, recv_in)
    found_copy = place_tiles(staged[6], found, where_tile, found_sem)
    w_pad[...] = jnp.zeros_like(w_pad)
    w_pad[0:classes, :] = w_outer[...]
    bias_col = jnp.broadcast_to(bias[...], (blk, hid)).T
    tile_copy.wait()
    found_copy.wait()
    aggregate(proj, out_in, got_in, send_in, recv_in, acc_in)
    score(acc_in, inv, bias_col, w_pad, scores, blk)
    deliver(scores, out_sc, got_sc, send_sc, recv_sc)
    aggregate(scores, out_sc, got_sc, send_sc, recv_sc, acc_sc)
    out[...] = inv * acc_sc[0:classes, :]

    @pl.loop(1, peers)
    def _(k):
        copy(out_in, got_in, send_in, recv_in, k).wait_send()
        copy(out_sc, got_sc, send_sc, recv_sc, k).wait_send()


def on_device(
    n_dom, n_sub,
    features, w_inner, bias_inner, w_outer, bias_outer, tiles, tile_col, degrees, send_rows
):
    peers = n_dom * n_sub
    verts, hid = features.shape[0], w_inner.shape[1]
    classes = w_outer.shape[1]
    padded = 16 * ((classes + 15) // 16)
    blk = tiles.shape[2]
    columns = verts // blk + peers
    lanes = 128 * ((columns + 127) // 128)
    small = (
        features.T, w_inner, bias_inner[None, :], w_outer.T, degrees[None, :], send_rows[0], tile_col
    )
    relay = n_sub == 4
    lists_out = 6 * n_dom if relay else peers
    vmem = pl.BlockSpec(memory_space=pltpu.VMEM)
    bf16, f32 = jnp.bfloat16, jnp.float32
    agg = pl.pallas_call(
        functools.partial(relay_kernel if relay else direct_kernel, n_dom, n_sub),
        out_shape=pltpu.VMEM((classes, verts), f32),
        in_specs=[pl.BlockSpec(memory_space=pl.ANY)] * 8,
        out_specs=vmem,
        scratch_shapes=[pltpu.VMEM(each.shape, each.dtype) for each in small]
        + [
            pltpu.SemaphoreType.DMA((len(small) + PARTS,)),
            pltpu.VMEM((tiles.shape[0], lanes), jnp.int32),
            pltpu.SMEM((tiles.shape[0], lanes), jnp.int32),
            pltpu.SemaphoreType.DMA,
            pltpu.VMEM((hid, verts), bf16),
            pltpu.VMEM((lists_out, hid, blk), bf16),
            pltpu.VMEM((peers, hid, blk), bf16),
            pltpu.VMEM((hid, verts), f32),
            pltpu.VMEM((padded, hid), bf16),
            pltpu.VMEM((padded, verts), bf16),
            pltpu.VMEM((peers + 2 * n_dom if relay else peers, padded, blk), bf16),
            pltpu.VMEM((peers, padded, blk), bf16),
            pltpu.VMEM((padded, verts), f32),
            pltpu.VMEM(tiles.shape, bf16),
            pltpu.SemaphoreType.DMA,
            pltpu.SemaphoreType.DMA((2 if relay else peers,)),
            pltpu.SemaphoreType.DMA((1 + 2 * HALVES + n_dom // 2 if relay else peers,)),
            pltpu.SemaphoreType.DMA if relay else pltpu.SemaphoreType.DMA((peers,)),
            pltpu.SemaphoreType.DMA((n_sub if relay else peers,)),
        ]
        + (
            [
                pltpu.VMEM((2, hid, verts), bf16),
                pltpu.VMEM((2, peers, blk), jnp.int32),
                pltpu.SemaphoreType.DMA,
                pltpu.SemaphoreType.DMA((2, HALVES)),
                pltpu.SemaphoreType.DMA,
                pltpu.SemaphoreType.DMA((2,)),
                pltpu.VMEM((columns, blk, verts), bf16),
                pltpu.VMEM((n_sub, verts, n_dom * blk), bf16),
                pltpu.SemaphoreType.REGULAR,
                pltpu.VMEM((2, 2, verts, n_dom * blk), bf16),
                pltpu.VMEM((2, padded, verts), bf16),
                pltpu.SemaphoreType.DMA,
                pltpu.SemaphoreType.DMA((2,)),
            ]
            if relay
            else []
        ),
        compiler_params=pltpu.CompilerParams(
            collective_id=0, has_side_effects=True, vmem_limit_bytes=56 * 1024 * 1024
        ),
    )(*small, tiles)
    return agg.T + bias_outer


def solution(mesh):
    return jax.shard_map(
        functools.partial(on_device, mesh.shape["dom"], mesh.shape["sub"]),
        mesh=mesh,
        in_specs=(
            P(("dom", "sub"), None),
            P(),
            P(),
            P(),
            P(),
            P(("dom", "sub"), None, None, None),
            P(("dom", "sub"), None),
            P(("dom", "sub")),
            P(("dom", "sub"), None, None),
        ),
        out_specs=P(("dom", "sub"), None),
        check_vma=False,
    )
```

```python
import functools

import jax
import jax.numpy as jnp
from jax import lax
from jax.experimental import pallas as pl
from jax.experimental.pallas import tpu as pltpu
from jax.sharding import PartitionSpec as P

MESH = pl.DeviceIdType.MESH
NT = (((1,), (1,)), ((), ()))
PARTS = 2
HALVES = 2


class Place:
    def __init__(self, n_dom, n_sub):
        self.n_dom, self.n_sub = n_dom, n_sub
        self.dom, self.sub = lax.axis_index("dom"), lax.axis_index("sub")
        self.mine = self.dom * n_sub + self.sub

    def flip(self, a):
        total, bit = 0, 1
        while bit < self.n_dom:
            total = total + lax.rem(lax.div(self.dom, bit) + lax.div(a, bit), 2) * bit
            bit *= 2
        return total

    def target(self, k):
        n_sub = self.n_sub
        return self.flip(lax.div(k, n_sub)), lax.rem(self.sub + lax.rem(k, n_sub), n_sub)

    def source(self, k):
        n_sub = self.n_sub
        return self.flip(lax.div(k, n_sub)) * n_sub + lax.rem(self.sub + n_sub - lax.rem(k, n_sub), n_sub)


def hot_of(first, second, lists, verts):
    slots = jnp.concatenate([lists[pl.ds(first, 1), :], lists[pl.ds(second, 1), :]], axis=1)
    hot = lax.broadcasted_iota(jnp.int32, (verts, slots.shape[1]), 0) == slots
    return jnp.where(hot, 1.0, 0.0).astype(jnp.bfloat16)


def taken(table, hot):
    return jnp.dot(table[...], hot, preferred_element_type=jnp.float32).astype(table.dtype)


def picked(first, second, table, lists):
    return taken(table, hot_of(first, second, lists, table.shape[-1]))


def add(acc, block, c0, c1, fresh, tiles, where_tile):
    rows, _, blk, _ = tiles.shape

    def tile(r, c):
        t = where_tile[r, c]
        found = tiles[r, jnp.maximum(t, 0)]
        return jnp.where(t >= 0, found, jnp.zeros_like(found))

    for r in range(0, rows, 2):
        weights = jnp.concatenate(
            [jnp.concatenate([tile(r + q, c0), tile(r + q, c1)], axis=1) for q in range(2)], axis=0
        )
        term = lax.dot_general(block, weights, NT, preferred_element_type=jnp.float32)
        span = slice(r * blk, (r + 2) * blk)
        acc[:, span] = term if fresh else acc[:, span] + term


def prologue(place, hbm, staged, tiles_hbm, tiles, tile_sem, stage_sem, proj, greet):
    ft, w_inner, _, _, degrees, _, _ = staged
    verts = proj.shape[1]
    part = verts // PARTS
    whole = ft.shape[0] // 256 * 256
    small = [
        pltpu.make_async_copy(src, dst, stage_sem.at[i])
        for i, (src, dst) in enumerate(zip(hbm, staged))
        if i
    ]
    wide = [
        pltpu.make_async_copy(
            hbm[0].at[:, pl.ds(v * part, part)], ft.at[:, pl.ds(v * part, part)], stage_sem.at[len(staged) + v]
        )
        for v in range(PARTS)
    ]
    small[0].start()
    small[3].start()
    for each in wide:
        each.start()
    for i in (1, 2, 4, 5):
        small[i].start()
    tile_copy = pltpu.make_async_copy(tiles_hbm, tiles, tile_sem)

    greet()

    small[0].wait()
    small[3].wait()
    inv = lax.rsqrt(degrees[...].astype(jnp.float32))
    w_t = w_inner[...].T
    for v in range(PARTS):
        span = slice(v * part, (v + 1) * part)
        wide[v].wait()
        term = jnp.dot(w_t[:, :whole], ft[:whole, span], preferred_element_type=jnp.float32)
        if whole < ft.shape[0]:
            term += jnp.dot(w_t[:, whole:], ft[whole:, span], preferred_element_type=jnp.float32)
        if v == PARTS - 1:
            tile_copy.start()
        proj[:, span] = (term * inv[:, span]).astype(proj.dtype)
    for i in (1, 2, 4, 5):
        small[i].wait()
    return inv, tile_copy


def place_tiles(tile_col, found, where_tile, found_sem):
    cols = tile_col[...]
    lane = lax.broadcasted_iota(jnp.int32, found.shape, 1)
    at = jnp.full(found.shape, -1, jnp.int32)
    for t in range(cols.shape[1]):
        at = jnp.where(cols[:, t:t + 1] == lane, t, at)
    found[...] = at
    found_copy = pltpu.make_async_copy(found, where_tile, found_sem)
    found_copy.start()
    return found_copy


def turn_of(i, count):
    return count - 1 - lax.div(i, 2) - count // 2 * lax.rem(i, 2)


def partner_of(i, count):
    a = turn_of(i, count)
    return a + 1 - 2 * lax.rem(a, 2)


def score(acc_in, inv, bias_col, w_pad, scores, blk):
    for v in range(0, scores.shape[1], blk):
        span = slice(v, v + blk)
        scale = inv[:, span]
        hidden = scale * jnp.maximum(scale * acc_in[:, span] + bias_col, 0.0)
        scores[:, span] = jnp.dot(
            w_pad[...], hidden.astype(jnp.bfloat16), preferred_element_type=jnp.float32
        ).astype(scores.dtype)


def relay_kernel(n_dom, n_sub, *refs):
    hbm, (tiles_hbm, out), staged, refs = refs[:7], refs[7:9], refs[9:16], refs[16:]
    (
        stage_sem, found, where_tile, found_sem, proj, out_in, got_in, acc_in, w_pad, scores, out_sc, got_sc,
        acc_sc, tiles, tile_sem, send_in, recv_in, send_sc, recv_sc, far_proj, far_lists, proj_send, proj_recv,
        lists_send, lists_recv, dense, hots, clear,
        passed_hots, far_scores, table_send, table_recv,
    ) = refs
    _, _, bias, w_outer, _, lists, _ = staged
    place = Place(n_dom, n_sub)
    dom, sub, flip = place.dom, place.sub, place.flip
    hid, verts = proj.shape
    blk = tiles.shape[2]
    own = verts // blk
    classes = w_outer.shape[0]
    part = hid // HALVES
    pairs = n_dom // 2
    per_step = 2 * n_dom
    peers = n_dom * n_sub
    half = lax.div(sub, 2)
    sibling, near, far = 1 + 4 * half - sub, 2 - half, 3 - 3 * half
    mid = lax.rem(sub + half, 2)
    middle, edge = mid == 1, mid == 0
    barrier = pltpu.get_barrier_semaphore()

    def greet():
        doms = [lax.rem(dom + d, n_dom) for d in range(n_dom)]
        for step in range(1, n_sub + 1):
            to_sub = lax.rem(sub + step, n_sub)
            for to_dom in doms[step // n_sub:]:
                pl.semaphore_signal(barrier, inc=1, device_id=(to_dom, to_sub), device_id_type=MESH)

    inv, tile_copy = prologue(place, hbm, staged, tiles_hbm, tiles, tile_sem, stage_sem, proj, greet)

    def lists_copy(slot):
        return pltpu.make_async_remote_copy(
            src_ref=lists, dst_ref=far_lists.at[slot], send_sem=lists_send, recv_sem=lists_recv.at[slot],
            device_id=(dom, near), device_id_type=MESH,
        )

    def piece_copy(slot, c):
        rows = pl.ds(c * part, part)
        return pltpu.make_async_remote_copy(
            src_ref=proj.at[rows], dst_ref=far_proj.at[slot, rows], send_sem=proj_send,
            recv_sem=proj_recv.at[slot, c], device_id=(dom, near), device_id_type=MESH,
        )

    def send_table(slot):
        lists_copy(slot).start()
        for c in range(HALVES):
            piece_copy(slot, c).start()

    def await_table():
        lists_copy(0).wait_send()
        pltpu.make_async_remote_copy(
            src_ref=proj, dst_ref=far_proj.at[0], send_sem=proj_send, recv_sem=proj_recv.at[0, 0],
            device_id=(dom, near), device_id_type=MESH,
        ).wait_send()

    def came_in(plane, m, c, slot):
        return recv_in.at[lax.rem(plane, 2) if c is None else 2 + HALVES * slot + c + (m if slot and c else 0)]

    def lists_of(ref, at, c):
        return ref.at[at] if c is None else ref.at[at, pl.ds(c * part, part)]

    def list_copy(j, plane, a, c, to_sub, slot=None):
        return pltpu.make_async_remote_copy(
            src_ref=lists_of(out_in, j, c), dst_ref=lists_of(got_in, plane * n_dom + a, c),
            send_sem=send_in.at[0 if slot is None else 1], recv_sem=came_in(plane, lax.div(a, 2), c, slot),
            device_id=(flip(a), to_sub), device_id_type=MESH,
        )

    def await_lists(plane, a, count, c, slot=None):
        pltpu.make_async_remote_copy(
            src_ref=lists_of(out_in, pl.ds(0, count), c),
            dst_ref=lists_of(got_in, pl.ds(plane * n_dom + a, count), c),
            send_sem=send_in.at[0], recv_sem=came_in(plane, lax.div(a, 2), c, slot),
            device_id=(dom, sibling), device_id_type=MESH,
        ).wait_recv()

    def await_sent(relayed, count):
        pltpu.make_async_remote_copy(
            src_ref=out_in.at[pl.ds(0, count)], dst_ref=out_in.at[pl.ds(0, count)],
            send_sem=send_in.at[relayed], recv_sem=recv_in.at[0],
            device_id=(dom, sibling), device_id_type=MESH,
        ).wait_send()

    def keep_hot(a, hot, first, second):
        at = pl.ds(pl.multiple_of(a * blk, blk), blk)
        hots[first, :, at] = hot[:, :blk]
        hots[second, :, at] = hot[:, blk:]

    def pick_own(a):
        row = flip(a) * n_sub
        hot = hot_of(row + sub, row + sibling, lists, verts)
        keep_hot(a, hot, sub, sibling)
        both = taken(proj, hot)
        out_in[2 * a + 1] = both[:, blk:]
        return both[:, :blk]

    def pick_both(a):
        mine = pick_own(a)
        out_in[2 * a] = mine

        @pl.when(a == 0)
        def _():
            got_in[sub * n_dom] = mine

    def send_both(a):
        list_copy(2 * a + 1, sub, a, None, sibling).start()
        pl.when(a != 0)(lambda: list_copy(2 * a, sub, a, None, sub).start())

    def hand_out_own():
        send_both(partner_of(0, n_dom))

        @pl.loop(1, n_dom)
        def _(i):
            a = partner_of(i, n_dom)
            pick_both(a)
            send_both(a)

    def turn(begin, end, column_of, at):
        def tile(r, c):
            t = where_tile[r, c]
            found = tiles[r, jnp.maximum(t, 0)]
            return jnp.where(t >= 0, found, jnp.zeros_like(found))

        @pl.loop(begin, end)
        def _(i):
            c = column_of(i)
            for r in range(0, tiles.shape[0], 2):
                both = jnp.concatenate([tile(r, c), tile(r + 1, c)], axis=0)
                dense[at + i, :, r * blk:(r + 2) * blk] = both.T

    def turn_slots(begin, end):
        turn(begin, end, lambda i: own + flip(lax.rem(i, n_dom)) * n_sub + lax.div(i, n_dom), own)

    def keep_far_hots():
        @pl.loop(0, n_dom)
        def _(a):
            row = flip(a) * n_sub
            keep_hot(a, hot_of(row + near, row + far, lists, verts), near, far)

    def relay(slot, c, plane):
        if c == 0:
            lists_copy(slot).wait_recv()
        piece_copy(slot, c).wait_recv()
        base = (slot + 1) * per_step
        rows = slice(c * part, (c + 1) * part)

        def pair(a):
            row = flip(a) * n_sub
            at = pl.ds(pl.multiple_of(a * blk, blk), blk)
            if c == 0:
                hot = hot_of(row + sub, row + sibling, far_lists.at[slot], verts)
                passed_hots[slot, 0, :, at] = hot[:, :blk]
                passed_hots[slot, 1, :, at] = hot[:, blk:]
            else:
                hot = jnp.concatenate([passed_hots[slot, 0, :, at], passed_hots[slot, 1, :, at]], axis=1)
            return taken(far_proj.at[slot, rows], hot)

        @pl.loop(0, n_dom)
        def _(i):
            a = partner_of(i, n_dom)
            both = pair(a)
            j = base + 2 * a
            out_in[j, rows, :] = both[:, :blk]
            out_in[j + 1, rows, :] = both[:, blk:]
            list_copy(j + 1, plane, a, c, sibling, slot).start()
            pl.when(a != 0)(lambda: list_copy(j, plane, a, c, sub, slot).start())

            @pl.when(a == 0)
            def _():
                got_in[plane * n_dom, rows, :] = both[:, :blk]

    def add_dense(acc, block, first, count, fresh):
        wide = 2 * blk if acc.shape[0] >= part else 8 * blk
        for v in range(0, verts, wide):
            span = slice(v, v + wide)
            weights = dense[pl.ds(first, count), :, span].reshape(count * blk, wide)
            term = jnp.dot(block, weights, preferred_element_type=jnp.float32)
            acc[:, span] = term if fresh else acc[:, span] + term

    def add_own(table, acc):
        add_dense(acc, table[...], 0, own, True)

    def add_pair(plane, m):
        slot = plane * n_dom + 2 * m
        add_dense(acc_in, jnp.concatenate([got_in[slot], got_in[slot + 1]], axis=1), own + slot, 2, False)

    def add_pairs(plane):
        @pl.loop(0, pairs)
        def _(i):
            add_pair(plane, turn_of(i, pairs))

    def add_plane(plane, local):
        await_lists(plane, local, n_dom - local, None)
        add_pairs(plane)

    def add_passed(slot, plane):
        await_lists(plane, 1, n_dom - 1, 0, slot)
        if slot:
            for m in range(pairs):
                await_lists(plane, 2 * m if m else 1, 2 if m else 1, 1, slot)
        else:
            await_lists(plane, 1, n_dom - 1, 1, slot)
        add_pairs(plane)

    def add_halves(slot, plane, c):
        rows = slice(c * part, (c + 1) * part)
        if not (slot and c):
            await_lists(plane, 0, n_dom, c, slot)

        @pl.loop(0, pairs)
        def _(i):
            m = turn_of(i, pairs)
            at = plane * n_dom + 2 * m
            if slot and c:
                await_lists(plane, 2 * m, 2, c, slot)
            block = jnp.concatenate([got_in[at, rows, :], got_in[at + 1, rows, :]], axis=1)
            add_dense(acc_in.at[rows], block, own + at, 2, False)

    pick_both(partner_of(0, n_dom))
    pl.semaphore_wait(barrier, peers - 1)
    pl.when(middle)(lambda: send_table(0))
    hand_out_own()
    found_copy = place_tiles(staged[6], found, where_tile, found_sem)
    w_pad[...] = jnp.zeros_like(w_pad)
    w_pad[0:classes, :] = w_outer[...]
    bias_col = jnp.broadcast_to(bias[...], (2 * blk, hid)).T
    tile_copy.wait()
    found_copy.wait()
    turn(0, own, lambda i: i, 0)
    turn_slots(0, n_dom)
    keep_far_hots()

    @pl.when(middle)
    def _():
        relay(0, 0, near)
        turn_slots(n_dom, 2 * n_dom)
        await_table()
        pl.semaphore_signal(clear, inc=1, device_id=(dom, sibling), device_id_type=MESH)
        turn_slots(2 * n_dom, peers)
        relay(0, 1, near)
        add_own(proj, acc_in)
        add_plane(sub, 1)
        relay(1, 0, far)
        add_plane(sibling, 0)
        relay(1, 1, far)
        add_passed(0, near)
        add_passed(1, far)

    @pl.when(edge)
    def _():
        turn_slots(n_dom, peers)
        add_own(proj, acc_in)
        pl.semaphore_wait(clear, 1)
        send_table(1)
        add_plane(sub, 1)
        add_plane(sibling, 0)
        add_halves(0, near, 0)
        add_halves(0, near, 1)
        add_halves(1, far, 0)
        add_halves(1, far, 1)

    score(acc_in, inv, bias_col, w_pad, scores, 2 * blk)

    order = [n_dom - 1 - i // 2 - n_dom // 2 * (i % 2) for i in range(n_dom)]
    order = [a + 1 - 2 * (a % 2) for a in order]

    def score_copy(k, source, a, plane):
        return pltpu.make_async_remote_copy(
            src_ref=out_sc.at[k], dst_ref=got_sc.at[source * n_dom + a], send_sem=send_sc,
            recv_sem=recv_sc.at[source], device_id=(flip(a), plane), device_id_type=MESH,
        )

    def give(table, hot_all, base, source, plane, local, pieces=n_dom):
        for i, a in enumerate(order):
            if i % pieces == 0:
                these = order[i:i + pieces]
                hot = hot_all[...] if pieces == n_dom else jnp.concatenate(
                    [hot_all[:, b * blk:(b + 1) * blk] for b in these], axis=1
                )
                lists_for = taken(table, hot)
            at = a if pieces == n_dom else i % pieces
            one = lists_for[:, at * blk:(at + 1) * blk]
            out_sc[base + a] = one
            if a or local is False:
                score_copy(base + a, source, a, plane).start()
            elif local is True:
                got_sc[source * n_dom] = one
            else:
                pl.when(jnp.logical_not(local))(lambda: score_copy(base, source, 0, plane).start())

                @pl.when(local)
                def _():
                    got_sc[source * n_dom] = one

    def deliver(plane, pieces=n_dom):
        give(scores, hots.at[plane], plane * n_dom, sub, plane, sub == plane, pieces)

    def table_copy(slot):
        return pltpu.make_async_remote_copy(
            src_ref=scores, dst_ref=far_scores.at[slot], send_sem=table_send, recv_sem=table_recv.at[slot],
            device_id=(dom, near), device_id_type=MESH,
        )

    def pass_scores(slot, source, to_own, to_sibling):
        table_copy(slot).wait_recv()
        give(far_scores.at[slot], passed_hots.at[slot, 1], to_sibling, source, sibling, False)
        give(far_scores.at[slot], passed_hots.at[slot, 0], to_own, source, sub, True)

    def scores_wait(at, count, plane):
        return pltpu.make_async_remote_copy(
            src_ref=out_sc.at[pl.ds(0, count)], dst_ref=got_sc.at[pl.ds(at, count)], send_sem=send_sc,
            recv_sem=recv_sc.at[plane], device_id=(dom, sibling), device_id_type=MESH,
        )

    def scores_sent(count):
        pltpu.make_async_remote_copy(
            src_ref=out_sc.at[pl.ds(0, count)], dst_ref=out_sc.at[pl.ds(0, count)], send_sem=send_sc,
            recv_sem=recv_sc.at[0], device_id=(dom, sibling), device_id_type=MESH,
        ).wait_send()

    def gather(plane):
        slot = plane * n_dom
        passed = jnp.logical_or(plane == near, jnp.logical_and(plane == 0, sub == 2))
        local = jnp.logical_or(plane == sub, jnp.logical_and(middle, passed))
        pl.when(jnp.logical_not(local))(lambda: scores_wait(slot, n_dom, plane).wait_recv())
        pl.when(local)(lambda: scores_wait(slot + 1, n_dom - 1, plane).wait_recv())
        block = jnp.concatenate([got_sc[slot + a] for a in range(n_dom)], axis=1)
        add_dense(acc_sc, block, own + slot, n_dom, False)

    @pl.when(middle)
    def _():
        table_copy(0).start()
        for plane in (sibling, sub):
            deliver(plane)

    @pl.when(sub == 0)
    def _():
        table_copy(1).start()
        deliver(sub)

    @pl.when(sub == 3)
    def _():
        deliver(far, n_dom // 2)
        for plane in (sub, near, sibling):
            deliver(plane)

    add_own(scores, acc_sc)
    await_sent(0, per_step - 1)
    pl.when(edge)(await_table)
    pl.when(middle)(lambda: pass_scores(0, near, near * n_dom, far * n_dom))
    pl.when(middle)(lambda: await_sent(1, 2 * (per_step - 1)))
    pl.when(sub == 0)(lambda: deliver(sibling))
    on = [lax.div(3 - sub, 3), 0, 0, lax.div(sub, 3)]
    on[1] = lax.rem(sub, 2) - on[3]
    on[2] = 1 - on[0] - on[1] - on[3]
    first, second, third, fourth = (
        sum(here * plane for here, plane in zip(on, planes))
        for planes in ((0, 1, 2, 2), (3, 2, 1, 1), (1, 0, 3, 3), (2, 3, 0, 0))
    )
    gather(first)
    pl.when(sub == 2)(lambda: pass_scores(1, 0, peers, peers + n_dom))
    gather(second)
    gather(third)
    gather(fourth)
    out[...] = inv * acc_sc[0:classes, :]

    @pl.when(sub == 0)
    def _():
        scores_sent(2 * n_dom - 1)

    pl.when(sub == 1)(lambda: scores_sent(peers - 2))
    pl.when(sub == 2)(lambda: scores_sent(peers + 2 * n_dom - 3))
    pl.when(sub == 3)(lambda: scores_sent(peers - 1))
    pl.when(sub != 3)(lambda: table_copy(0).wait_send())


def direct_kernel(n_dom, n_sub, *refs):
    hbm, (tiles_hbm, out), staged, refs = refs[:7], refs[7:9], refs[9:16], refs[16:]
    (
        stage_sem, found, where_tile, found_sem, proj, out_in, got_in, acc_in, w_pad, scores, out_sc, got_sc,
        acc_sc, tiles, tile_sem, send_in, recv_in, send_sc, recv_sc,
    ) = refs
    _, _, bias, w_outer, _, lists, _ = staged
    place = Place(n_dom, n_sub)
    peers = n_dom * n_sub
    hid, verts = proj.shape
    blk = tiles.shape[2]
    own = verts // blk
    classes = w_outer.shape[0]

    barrier = pltpu.get_barrier_semaphore()

    def greet():
        @pl.loop(1, peers)
        def _(k):
            pl.semaphore_signal(barrier, inc=1, device_id=place.target(k), device_id_type=MESH)

    inv, tile_copy = prologue(place, hbm, staged, tiles_hbm, tiles, tile_sem, stage_sem, proj, greet)
    pl.semaphore_wait(barrier, peers - 1)

    def copy(src, dst, sends, recvs, k):
        return pltpu.make_async_remote_copy(
            src_ref=src.at[k], dst_ref=dst.at[k], send_sem=sends.at[k], recv_sem=recvs.at[k],
            device_id=place.target(k), device_id_type=MESH,
        )

    def pick(k, table):
        index = [to_dom * n_sub + to_sub for to_dom, to_sub in (place.target(k), place.target(k + 1))]
        return picked(*index, table, lists)

    def deliver(table, outgoing, got, sends, recvs):
        first = pick(0, table)
        got[0] = first[:, :blk]
        outgoing[1] = first[:, blk:]
        copy(outgoing, got, sends, recvs, 1).start()

        @pl.loop(1, peers // 2)
        def _(pair):
            k = 2 * pair
            both = pick(k, table)
            outgoing[k] = both[:, :blk]
            outgoing[k + 1] = both[:, blk:]
            copy(outgoing, got, sends, recvs, k).start()
            copy(outgoing, got, sends, recvs, k + 1).start()

    def aggregate(table, outgoing, got, sends, recvs, acc):
        for c in range(0, own, 2):
            add(acc, table[:, c * blk:(c + 2) * blk], c, c + 1, c == 0, tiles, where_tile)

        def arrived(k):
            block = jnp.concatenate([got[k], got[k + 1]], axis=1)
            add(acc, block, own + place.source(k), own + place.source(k + 1), False, tiles, where_tile)

        copy(outgoing, got, sends, recvs, 1).wait_recv()
        arrived(0)

        @pl.loop(1, peers // 2)
        def _(pair):
            k = 2 * pair
            copy(outgoing, got, sends, recvs, k).wait_recv()
            copy(outgoing, got, sends, recvs, k + 1).wait_recv()
            arrived(k)

    deliver(proj, out_in, got_in, send_in, recv_in)
    found_copy = place_tiles(staged[6], found, where_tile, found_sem)
    w_pad[...] = jnp.zeros_like(w_pad)
    w_pad[0:classes, :] = w_outer[...]
    bias_col = jnp.broadcast_to(bias[...], (2 * blk, hid)).T
    tile_copy.wait()
    found_copy.wait()
    aggregate(proj, out_in, got_in, send_in, recv_in, acc_in)
    score(acc_in, inv, bias_col, w_pad, scores, 2 * blk)
    deliver(scores, out_sc, got_sc, send_sc, recv_sc)
    aggregate(scores, out_sc, got_sc, send_sc, recv_sc, acc_sc)
    out[...] = inv * acc_sc[0:classes, :]

    @pl.loop(1, peers)
    def _(k):
        copy(out_in, got_in, send_in, recv_in, k).wait_send()
        copy(out_sc, got_sc, send_sc, recv_sc, k).wait_send()


def on_device(
    n_dom, n_sub,
    features, w_inner, bias_inner, w_outer, bias_outer, tiles, tile_col, degrees, send_rows
):
    peers = n_dom * n_sub
    verts, hid = features.shape[0], w_inner.shape[1]
    classes = w_outer.shape[1]
    padded = 16 * ((classes + 15) // 16)
    blk = tiles.shape[2]
    columns = verts // blk + peers
    lanes = 128 * ((columns + 127) // 128)
    small = (
        features.T, w_inner, bias_inner[None, :], w_outer.T, degrees[None, :], send_rows[0], tile_col
    )
    relay = n_sub == 4
    lists_out = 6 * n_dom if relay else peers
    vmem = pl.BlockSpec(memory_space=pltpu.VMEM)
    bf16, f32 = jnp.bfloat16, jnp.float32
    agg = pl.pallas_call(
        functools.partial(relay_kernel if relay else direct_kernel, n_dom, n_sub),
        out_shape=pltpu.VMEM((classes, verts), f32),
        in_specs=[pl.BlockSpec(memory_space=pl.ANY)] * 8,
        out_specs=vmem,
        scratch_shapes=[pltpu.VMEM(each.shape, each.dtype) for each in small]
        + [
            pltpu.SemaphoreType.DMA((len(small) + PARTS,)),
            pltpu.VMEM((tiles.shape[0], lanes), jnp.int32),
            pltpu.SMEM((tiles.shape[0], lanes), jnp.int32),
            pltpu.SemaphoreType.DMA,
            pltpu.VMEM((hid, verts), bf16),
            pltpu.VMEM((lists_out, hid, blk), bf16),
            pltpu.VMEM((peers, hid, blk), bf16),
            pltpu.VMEM((hid, verts), f32),
            pltpu.VMEM((padded, hid), bf16),
            pltpu.VMEM((padded, verts), bf16),
            pltpu.VMEM((peers + 2 * n_dom if relay else peers, padded, blk), bf16),
            pltpu.VMEM((peers, padded, blk), bf16),
            pltpu.VMEM((padded, verts), f32),
            pltpu.VMEM(tiles.shape, bf16),
            pltpu.SemaphoreType.DMA,
            pltpu.SemaphoreType.DMA((2 if relay else peers,)),
            pltpu.SemaphoreType.DMA((1 + 2 * HALVES + n_dom // 2 if relay else peers,)),
            pltpu.SemaphoreType.DMA if relay else pltpu.SemaphoreType.DMA((peers,)),
            pltpu.SemaphoreType.DMA((n_sub if relay else peers,)),
        ]
        + (
            [
                pltpu.VMEM((2, hid, verts), bf16),
                pltpu.VMEM((2, peers, blk), jnp.int32),
                pltpu.SemaphoreType.DMA,
                pltpu.SemaphoreType.DMA((2, HALVES)),
                pltpu.SemaphoreType.DMA,
                pltpu.SemaphoreType.DMA((2,)),
                pltpu.VMEM((columns, blk, verts), bf16),
                pltpu.VMEM((n_sub, verts, n_dom * blk), bf16),
                pltpu.SemaphoreType.REGULAR,
                pltpu.VMEM((2, 2, verts, n_dom * blk), bf16),
                pltpu.VMEM((2, padded, verts), bf16),
                pltpu.SemaphoreType.DMA,
                pltpu.SemaphoreType.DMA((2,)),
            ]
            if relay
            else []
        ),
        compiler_params=pltpu.CompilerParams(
            collective_id=0, has_side_effects=True, vmem_limit_bytes=56 * 1024 * 1024
        ),
    )(*small, tiles)
    return agg.T + bias_outer


def solution(mesh):
    return jax.shard_map(
        functools.partial(on_device, mesh.shape["dom"], mesh.shape["sub"]),
        mesh=mesh,
        in_specs=(
            P(("dom", "sub"), None),
            P(),
            P(),
            P(),
            P(),
            P(("dom", "sub"), None, None, None),
            P(("dom", "sub"), None),
            P(("dom", "sub")),
            P(("dom", "sub"), None, None),
        ),
        out_specs=P(("dom", "sub"), None),
        check_vma=False,
    )
```
